32 devices in a mesh: row: 2 (over y), col: 4 (over z), depth: 4 (over x, core).
Axes of the slice: x: 2, y: 2, z: 4, core: 2. Of those that a mesh axis runs over, the one named last changes fastest.
Arguments:
- matrix: float32 [8, 2, 512, 8192], P(None, 'row', None, ('col', 'depth')), as said below
Outputs:
- factored: float32 [8, 2, 512, 8192], P(None, 'row', None, ('col', 'depth'))
Inputs may be any that keep to these rules, and one draw needn't show every extreme that they name: matrix is symmetric positive definite.
All inputs are finite; a program needn't handle non-finite values.
Results may differ from the reference program's by a relative error of at most 0.0001.
Values sent between devices are 32-bit elements; how exact they have to be, the bound alone decides.
A program may use at most 128 MiB of HBM per device.

```python
import math
import jax
import jax.numpy as jnp
from jax import lax

B = 512
PANELS = 2
RB = 8
NBLK = 16
ORDER = 8192
N_ROW = 2


def draw_matrix(key, part):
    key_normal = jax.random.fold_in(key, 11)
    key_diagonal = jax.random.fold_in(key, 12)
    latent = 4 * B
    gaussian = jax.random.normal(key_normal, (ORDER, latent), jnp.float32)
    product = jnp.dot(gaussian, gaussian.T, precision=lax.Precision.HIGHEST) / math.sqrt(latent)
    symmetric = (product + product.T) * 0.5
    diag_shift = jax.random.uniform(key_diagonal, (ORDER,), jnp.float32, 0.1, 0.3) * math.sqrt(latent)
    positions = jnp.arange(ORDER)
    symmetric = symmetric.at[positions, positions].add(diag_shift)
    return symmetric.reshape(RB, N_ROW, B, ORDER)


def setup_inputs(seed: int = 0) -> dict:
    seeds = jax.random.split(jax.random.key(seed), 2)
    return {
        "matrix": draw_matrix(jax.random.fold_in(seeds[1], 71), 0),
    }


def factor_blocks(lower_factor, blocks, block_ids, panel_index):
    count_rows, block_size, _ = blocks.shape
    solved = lax.linalg.triangular_solve(lower_factor, blocks.reshape(count_rows * block_size, block_size), left_side=False, lower=True, transpose_a=True)
    solved = solved.reshape(count_rows, block_size, block_size)
    marks = block_ids[:, None, None]
    return jnp.where(marks > panel_index, solved, jnp.where(marks == panel_index, lower_factor[None], jnp.float32(0.0)))

def reference(matrix):
    matrix_full = matrix.reshape(ORDER, ORDER)
    for panel_index in range(PANELS):
        start_col = panel_index * B
        stop_col = start_col + B
        lower_factor = jnp.linalg.cholesky(matrix_full[start_col:stop_col, start_col:stop_col])
        blocks = matrix_full[:, start_col:stop_col].reshape(NBLK, B, B)
        panel_full = factor_blocks(lower_factor, blocks, jnp.arange(NBLK, dtype=jnp.int32), panel_index).reshape(ORDER, B)
        trailing = matrix_full[:, stop_col:] - jnp.dot(panel_full, panel_full[stop_col:].T, precision=lax.Precision.HIGHEST)
        below_rows = (jnp.arange(ORDER, dtype=jnp.int32) >= stop_col)[:, None]
        trailing = jnp.where(below_rows, trailing, jnp.float32(0.0))
        matrix_full = jnp.concatenate([matrix_full[:, :start_col], panel_full, trailing], axis=1)
    return matrix_full.reshape(RB, N_ROW, B, ORDER)
```

```python
import functools

import jax
import jax.numpy as jnp
from jax import lax
from jax.experimental import pallas as pl
from jax.experimental.pallas import tpu as pltpu
from jax.sharding import PartitionSpec as P

PANELS = 2
MESH = pl.DeviceIdType.MESH
HI = lax.Precision.HIGHEST
T = 128
NT = (((1,), (1,)), ((), ()))
TN = (((0,), (0,)), ((), ()))
NN = (((1,), (0,)), ((), ()))
DIAGS = ((0, 0), (0, 1), (1, 1))


def dot(a, b, dims=NN):
    return lax.dot_general(a, b, dims, precision=HI, preferred_element_type=jnp.float32)


def factor_tile(aug):
    def strip(i, carry):
        j0 = pl.multiple_of(i * 8, 8)
        rows = aug[pl.ds(j0, 8), :]
        lane = lax.broadcasted_iota(jnp.int32, (8, T), 1)
        sub = lax.broadcasted_iota(jnp.int32, (8, T), 0)
        sub2 = lax.broadcasted_iota(jnp.int32, (8, 2 * T), 0)
        left = rows[:, :T]
        cols = [
            jnp.broadcast_to(
                jnp.sum(jnp.where(lane == j0 + t, left, 0.0), axis=1, keepdims=True), (8, T)
            )
            for t in range(8)
        ]
        for t in range(8):
            p = cols[t][t : t + 1, :]
            r = lax.rsqrt(p)
            r = r * (1.5 - 0.5 * p * r * r)
            coef = cols[t] * r
            for u in range(t + 1, 8):
                head = cols[u][t : t + 1, :] * r
                cols[u] = jnp.where(sub > t, cols[u] - coef * head, cols[u])
            wide_r = jnp.concatenate([r, r], axis=1)
            wide_c = jnp.concatenate([coef, coef], axis=1)
            head = rows[t : t + 1, :] * wide_r
            rows = jnp.where(sub2 == t, head, jnp.where(sub2 > t, rows - wide_c * head, rows))
        aug[pl.ds(j0, 8), :] = rows
        later = jnp.where(lane >= j0 + 8, rows[:, :T], 0.0)
        aug[...] -= dot(later, rows, TN)
        return carry

    lax.fori_loop(0, T // 8, strip, 0)


def split(x):
    top = x.astype(jnp.bfloat16)
    return top, (x - top.astype(jnp.float32)).astype(jnp.bfloat16)


def dot3(left, right, dims=NN):
    acc = None
    for a, b in ((left[1], right[0]), (left[0], right[1]), (left[0], right[0])):
        term = lax.dot_general(a, b, dims, preferred_element_type=jnp.float32)
        acc = term if acc is None else acc + term
    return acc


def kernel(
    shape, first, m_ref, o_ref,
    xs, mbuf, diag, work, aug, w, u01, ufix, cross, y0, y1, z0, bt, top, low,
    dsend, drecv, dloc, xsend, xrecv, csend, crecv, cloc, wsend, wrecv, mload, osend,
):
    n_row, n_col, n_dep = shape
    slots, block, _ = m_ref.shape
    held = slots - first
    half = block // 2
    n_dc = block // T
    n_pair = n_dep // 2
    r = lax.axis_index("row")
    c = lax.axis_index("col")
    d = lax.axis_index("depth")
    j = c * n_dep + d
    sib = d + 1 - 2 * lax.rem(d, 2)
    comm = lax.rem(d, 2) == lax.rem(r, 2)
    chain = jnp.logical_not(comm)
    kr = jnp.minimum(r, PANELS - 1)

    def dest(rr=None, cc=None, dd=None):
        return (r if rr is None else rr, c if cc is None else cc, d if dd is None else dd)

    def remote(src, dst, send, recv, to):
        return pltpu.make_async_remote_copy(
            src_ref=src, dst_ref=dst, send_sem=send, recv_sem=recv,
            device_id=to, device_id_type=MESH,
        )

    def chunks(n):
        if n == 1:
            return [(g * T, 0, block) for g in range(n_dc)]
        out = [(g * T, g * T, block - g * T) for g in range(n_dc)]
        if n == 0:
            out[:1] = [(0, 0, T), (0, T, block - T)]
        return out

    def diag_part(ref, n, g):
        at, col, wide = chunks(n)[g]
        return ref.at[pl.ds(at, T), pl.ds(col, wide)]

    def diag_copy(n, g, lane, to):
        part = diag_part(diag.at[n], n, g)
        return remote(part, part, dsend.at[n, g, lane], drecv.at[n, g], to)

    def diag_load(n, g):
        return pltpu.make_async_copy(
            diag_part(m_ref.at[0], n, g), diag_part(diag.at[n], n, g), dloc.at[n, g]
        )

    def diag_roles(n):
        row, k = DIAGS[n]
        root = (r == row) & (c == 0) & (d == k)
        own_entry = row % 2 == k % 2
        near = d < 2
        entry = comm & near & (c == 0) & (r == row)
        out = [(0, comm & near & (c < n_col - 1), dest(cc=lax.rem(c + 1, n_col)))]
        for q in range(1, n_pair):
            out.append((1 + q, comm & near, dest(dd=lax.rem(d + 2 * q, n_dep))))
        for step in range(1, n_row):
            rr = lax.rem(r + step, n_row)
            out.append((n_pair + step, entry, dest(rr=rr, dd=lax.rem(rr, 2))))
        down = comm if own_entry else ((comm & jnp.logical_not(entry)) | root)
        out.insert(0, (1, down, dest(dd=sib)))
        rows = [x for x in out if x[0] > n_pair]
        rest = [x for x in out if x[0] <= n_pair]
        return root, rows + rest

    def diag_step(n, g):
        root, out = diag_roles(n)

        @pl.when(root)
        def _():
            diag_load(n, g).wait()

        @pl.when(jnp.logical_not(root))
        def _():
            diag_copy(n, g, 0, dest(dd=sib)).wait_recv()

        for lane, cond, to in out:
            @pl.when(cond)
            def _():
                diag_copy(n, g, lane, to).start()

    def diag_relay(n):
        for g in range(len(chunks(n))):
            diag_step(n, g)

    def diag_drain(n):
        _, out = diag_roles(n)
        for g in range(len(chunks(n))):
            for lane, cond, to in out:
                @pl.when(cond)
                def _():
                    diag_copy(n, g, lane, to).wait_send()

    def cross_copy(step):
        return remote(
            m_ref.at[0], cross.at[kr], csend.at[step - 1], crecv.at[kr],
            dest(rr=lax.rem(r + step, n_row)),
        )

    def cross_local():
        return pltpu.make_async_copy(m_ref.at[0], cross.at[kr], cloc.at[0])

    def cross_start():
        @pl.when(r < PANELS)
        def _():
            cross_local().start()
            for step in range(1, n_row):
                cross_copy(step).start()

    def cross_wait(k):
        @pl.when(k == r)
        def _():
            cross_local().wait()

        @pl.when(k != r)
        def _():
            remote(
                m_ref.at[0], cross.at[k], csend.at[0], crecv.at[k],
                dest(rr=lax.rem(r + 1, n_row)),
            ).wait_recv()

    def piece(s, side, step):
        cs = c - side * s
        ds = lax.rem(d + 2 * step, n_dep)
        col = jnp.clip(cs, 0, n_col - 1) * n_dep + ds
        a = col // n_row
        ok = comm & (cs >= 0) & (cs < n_col) & (lax.rem(col, n_row) == r) & (a >= first)
        return ok, jnp.clip(a - first, 0, held - 1)

    def piece_out(s, side, step):
        out = []
        if step == 0:
            if side == 1 or s == 0:
                out.append((0, c < n_col - 1, dest(cc=lax.rem(c + 1, n_col))))
            if side == -1 or s == 0:
                out.append((1, c > 0, dest(cc=lax.rem(c + n_col - 1, n_col))))
            for q in range(1, n_pair):
                out.append((2 + q, c >= 0, dest(dd=lax.rem(d + 2 * q, n_dep))))
        out.append((2, c >= 0, dest(dd=sib)))
        return out

    def x_part(k, a, h):
        return xs.at[k, a, pl.ds(pl.multiple_of(h * half, half), half), :]

    def x_copy(k, a, h, lane, to):
        part = x_part(k, a, h)
        return remote(part, part, xsend.at[k, a, h, lane], xrecv.at[k, a, h], to)

    def x_event(s, side, step, k):
        ok, a = piece(s, side, step)

        @pl.when(ok)
        def _():
            def part(h, carry):
                if s > 0 or step > 0:
                    x_copy(k, a, h, 2, dest(dd=sib)).wait_recv()
                for lane, cond, to in piece_out(s, side, step):
                    @pl.when(cond)
                    def _():
                        x_copy(k, a, h, lane, to).start()
                return carry

            lax.fori_loop(0, 2, part, 0)

    places = [(0, 1)] + [(s, side) for s in range(1, n_col) for side in (1, -1)]

    def x_own(k):
        ok, a = piece(0, 1, 0)

        @pl.when(ok)
        def _():
            def turn(e, carry):
                i = pl.multiple_of((e // n_dc) * T, T)
                l = pl.multiple_of(lax.rem(e, n_dc) * T, T)
                xs[k, a, pl.ds(l, T), pl.ds(i, T)] = cross[k, pl.ds(i, T), pl.ds(l, T)].T
                return carry

            lax.fori_loop(0, n_dc * n_dc, turn, 0)

    def x_drain():
        def one(e, carry):
            k = e // 2
            h = lax.rem(e, 2)
            for s, side in places:
                for step in range(n_pair):
                    ok, a = piece(s, side, step)
                    for lane, cond, to in piece_out(s, side, step):
                        @pl.when(ok & cond)
                        def _():
                            x_copy(k, a, h, lane, to).wait_send()
            return carry

        lax.fori_loop(0, 2 * PANELS, one, 0)

    def w_copy(panel, b):
        rows = pl.ds(pl.multiple_of(b * T, T), T)
        part = w.at[panel, rows, :]
        return remote(part, part, wsend.at[panel, b], wrecv.at[panel, b], dest(dd=sib))

    def u_copy():
        return remote(u01, u01, wsend.at[PANELS, 0], wrecv.at[PANELS, 0], dest(dd=sib))

    def fix_copy():
        return remote(ufix, ufix, wsend.at[PANELS, 1], wrecv.at[PANELS, 1], dest(dd=sib))

    def m_load(s):
        return pltpu.make_async_copy(m_ref.at[s + first], mbuf.at[s + first], mload.at[s])

    def all_loads(wait):
        def one(s, carry):
            if wait:
                m_load(s).wait()
            else:
                m_load(s).start()
            return carry

        lax.fori_loop(0, held, one, 0)

    for n, (row, k) in enumerate(DIAGS):
        @pl.when((d == k) & (c == 0) & (r == row))
        def _():
            for g in range(len(chunks(n))):
                diag_load(n, g).start()

    def eye(rows, columns, at):
        i = lax.broadcasted_iota(jnp.int32, (rows, columns), 0)
        l = lax.broadcasted_iota(jnp.int32, (rows, columns), 1)
        return jnp.where(i + at == l, jnp.float32(1.0), jnp.float32(0.0))

    def upper(x, at):
        i = lax.broadcasted_iota(jnp.int32, x.shape, 0)
        l = lax.broadcasted_iota(jnp.int32, x.shape, 1)
        return jnp.where(i + at <= l, x, 0.0)

    def lower(x, at):
        i = lax.broadcasted_iota(jnp.int32, x.shape, 0)
        l = lax.broadcasted_iota(jnp.int32, x.shape, 1)
        return jnp.where(i + at >= l, x, 0.0)

    def each_tile(f, size=T):
        def step(e, carry):
            f(pl.multiple_of(e * size, size))
            return carry

        lax.fori_loop(0, block // size, step, 0)

    @pl.when(comm)
    def _():
        diag_relay(0)
        cross_start()
        for kk in range(PANELS):
            k = lax.rem(r + kk, PANELS)
            cross_wait(k)
            x_own(k)
            for step in range(n_pair):
                x_event(0, 1, step, k)
            diag_relay(1 + kk)
        all_loads(False)
        for s in range(1, n_col):
            for kk in range(PANELS):
                k = lax.rem(r + kk, PANELS)
                for side in (1, -1):
                    for step in range(n_pair):
                        x_event(s, side, step, k)
        for b in range(n_dc):
            w_copy(0, b).wait_recv()
        u_copy().wait_recv()

    def factor_block(panel):
        def tile(b, carry):
            at = pl.multiple_of(b * T, T)
            rows = pl.ds(at, T)
            aug[:, :T] = work[rows, rows]
            aug[:, T:] = eye(T, T, 0)
            factor_tile(aug)
            if panel == 0:
                @pl.when(b == 0)
                def _():
                    for g in range(1, n_dc + 1):
                        diag_step(0, g)
                    each_tile(fill)
            line = dot(aug[:, T:], work[rows, :])
            work[rows, :] = line
            w[panel, rows, :] = lower(line[:, block:], at)

            @pl.when(r == panel)
            def _():
                ufix[rows, :] = upper(line[:, :block], at)

            @pl.when(b < n_dc - 1)
            def _():
                lane = lax.broadcasted_iota(jnp.int32, (T, block), 1)
                aside = jnp.where(lane >= at + T, line[:, :block], 0.0)

                def tail(e, carry2):
                    cols = pl.ds(pl.multiple_of(e * 2 * T, 2 * T), 2 * T)
                    work[:, cols] -= dot(aside, work[rows, cols], TN)
                    return carry2

                lax.fori_loop(0, block // T, tail, 0)

            w_copy(panel, b).start()
            return carry

        lax.fori_loop(0, n_dc, tile, 0)

    def fill(at):
        rows = pl.ds(at, T)
        work[rows, :block] = diag[0, rows, :]
        work[rows, block:] = eye(T, block, at)

    def join(at):
        rows = pl.ds(at, T)
        u01[rows, :] = dot(w[0, rows, :], diag[1])

    def second(at):
        rows = pl.ds(at, T)
        work[rows, :block] = diag[2, rows, :] - dot(u01[:, rows], u01[...], TN)
        work[rows, block:] = eye(T, block, at)

    @pl.when(chain)
    def _():
        cross_start()
        diag_step(0, 0)
        work[pl.ds(0, T), pl.ds(0, T)] = diag[0, pl.ds(0, T), pl.ds(0, T)]
        all_loads(False)
        diag_start = DIAGS[1]

        @pl.when((r == diag_start[0]) & (c == 0) & (d == diag_start[1]))
        def _():
            diag_relay(1)

        factor_block(0)

        @pl.when(jnp.logical_not((r == diag_start[0]) & (c == 0) & (d == diag_start[1])))
        def _():
            diag_relay(1)

        each_tile(join)
        u_copy().start()
        diag_relay(2)
        each_tile(second)
        factor_block(1)
        for k in range(PANELS):
            cross_wait(jnp.int32(k))

        @pl.when(r < PANELS)
        def _():
            fix_copy().start()

    def unit(k, x, at):
        i1 = lax.broadcasted_iota(jnp.int32, x.shape, 0)
        i2 = lax.broadcasted_iota(jnp.int32, x.shape, 1)
        minus = jnp.where((i1 + at == i2) & (j == k), jnp.float32(-1.0), 0.0)
        return jnp.where(j < PANELS, minus, x)

    def cut(ref, *index):
        return split(ref[index])

    def s1(at):
        rows = pl.ds(at, half)
        y0[rows, :] = unit(0, dot3(split(w[0, rows, :]), split(cross[0])), at)

    def s2(at):
        rows = pl.ds(at, half)
        y1[rows, :] = cross[1, rows, :] - dot3(split(u01[:, rows]), split(y0[...]), TN)

    def s3(at):
        rows = pl.ds(at, half)
        z0[rows, :] = dot3(split(w[0, :, rows]), split(y0[...]), TN)
        bt[rows, :] = dot3(split(w[0, :, rows]), split(u01[...]), TN)

    def s4(at):
        rows = pl.ds(at, half)
        y0[rows, :] = unit(1, dot3(split(w[1, rows, :]), split(y1[...])), at)

    def s5(at):
        rows = pl.ds(at, half)
        value = dot3(split(w[1, :, rows]), split(y0[...]), TN)
        top[1, rows, :], low[1, rows, :] = split(value)

    def s6(at):
        rows = pl.ds(at, half)
        value = z0[rows, :] - dot3(split(bt[rows, :]), (top[1], low[1]))
        top[0, rows, :], low[0, rows, :] = split(value)

    each_tile(s1, half)
    each_tile(s2, half)
    each_tile(s3, half)

    @pl.when(comm)
    def _():
        for b in range(n_dc):
            w_copy(1, b).wait_recv()

    each_tile(s4, half)
    each_tile(s5, half)
    each_tile(s6, half)

    @pl.when(chain)
    def _():
        def arrive(e, carry):
            x_copy(e // (2 * held), lax.rem(e // 2, held), lax.rem(e, 2), 2, dest(dd=sib)).wait_recv()
            return carry

        lax.fori_loop(0, PANELS * held * 2, arrive, 0)

    all_loads(True)

    def out_copy(s, h):
        rows = pl.ds(pl.multiple_of(h * half, half), half)
        return pltpu.make_async_copy(mbuf.at[s, rows, :], o_ref.at[s, rows, :], osend.at[s, h])

    def update(e, carry):
        a = e // 2
        h = lax.rem(e, 2)
        rows = pl.ds(pl.multiple_of(h * half, half), half)
        acc = jnp.where(j >= PANELS, mbuf[a + first, rows, :], 0.0)
        for k in range(PANELS):
            acc = acc - dot3(split(xs[k, a, rows, :]), (top[k], low[k]))
        mbuf[a + first, rows, :] = acc
        if first:
            out_copy(a + first, h).start()
        else:
            @pl.when((a > 0) | (r >= PANELS))
            def _():
                out_copy(a, h).start()
        return carry

    lax.fori_loop(0, 2 * held, update, 0)

    @pl.when(r < PANELS)
    def _():
        @pl.when(comm)
        def _():
            fix_copy().wait_recv()

        mbuf[0] = jnp.zeros((block, block), jnp.float32)

        def turned(ref):
            def turn(e, carry):
                i = pl.multiple_of((e // n_dc) * T, T)
                l = pl.multiple_of(lax.rem(e, n_dc) * T, T)
                mbuf[0, pl.ds(l, T), pl.ds(i, T)] = ref[pl.ds(i, T), pl.ds(l, T)].T
                return carry

            lax.fori_loop(0, n_dc * n_dc, turn, 0)

        @pl.when(j == r)
        def _():
            turned(ufix)

        @pl.when((j == 0) & (r == 1))
        def _():
            turned(u01)

        for h in range(2):
            out_copy(0, h).start()

    if first:
        pass

    @pl.when(r < PANELS)
    def _():
        for step in range(1, n_row):
            cross_copy(step).wait_send()

    @pl.when(chain)
    def _():
        for panel in range(PANELS):
            for b in range(n_dc):
                w_copy(panel, b).wait_send()
        u_copy().wait_send()

        @pl.when(r < PANELS)
        def _():
            fix_copy().wait_send()

    for n in range(len(DIAGS)):
        diag_drain(n)
    x_drain()

    def finish(e, carry):
        out_copy(e // 2, lax.rem(e, 2)).wait()
        return carry

    lax.fori_loop(0, 2 * slots, finish, 0)


def body(shape, matrix):
    n_row, n_col, n_dep = shape
    m = matrix.reshape(matrix.shape[0], matrix.shape[2], matrix.shape[3])
    slots, block, _ = m.shape
    first = 1 if n_row <= PANELS else 0
    held = slots - first
    n_dc = block // T
    n_pair = n_dep // 2
    f32 = jnp.float32
    dma = pltpu.SemaphoreType.DMA
    hbm = pl.BlockSpec(memory_space=pltpu.HBM)
    square = pltpu.VMEM((block, block), f32)
    out = pl.pallas_call(
        functools.partial(kernel, shape, first),
        out_shape=jax.ShapeDtypeStruct(m.shape, f32),
        in_specs=[hbm],
        out_specs=hbm,
        scratch_shapes=[
            pltpu.VMEM((PANELS, held, block, block), f32),
            pltpu.VMEM((slots, block, block), f32),
            pltpu.VMEM((len(DIAGS), block, block), f32),
            pltpu.VMEM((block, 2 * block), f32),
            pltpu.VMEM((T, 2 * T), f32),
            pltpu.VMEM((PANELS, block, block), f32),
            square, square,
            pltpu.VMEM((PANELS, block, block), f32),
            square, square, square, square,
            pltpu.VMEM((PANELS, block, block), jnp.bfloat16),
            pltpu.VMEM((PANELS, block, block), jnp.bfloat16),
            dma((len(DIAGS), n_dc + 1, n_pair + n_row)),
            dma((len(DIAGS), n_dc + 1)),
            dma((len(DIAGS), n_dc + 1)),
            dma((PANELS, held, 2, 2 + n_pair)),
            dma((PANELS, held, 2)),
            dma((n_row - 1,)),
            dma((PANELS,)),
            dma((1,)),
            dma((PANELS + 1, n_dc)),
            dma((PANELS + 1, n_dc)),
            dma((held,)),
            dma((slots, 2)),
        ],
        compiler_params=pltpu.CompilerParams(has_side_effects=True, vmem_limit_bytes=60 << 20),
    )(m)
    return out.reshape(matrix.shape)


def solution(mesh):
    shape = (mesh.shape["row"], mesh.shape["col"], mesh.shape["depth"])
    placed = P(None, "row", None, ("col", "depth"))
    return jax.shard_map(
        functools.partial(body, shape),
        mesh=mesh,
        in_specs=(placed,),
        out_specs=placed,
        check_vma=False,
    )
```

```python
import functools

import jax
import jax.numpy as jnp
from jax import lax
from jax.experimental import pallas as pl
from jax.experimental.pallas import tpu as pltpu
from jax.sharding import PartitionSpec as P

PANELS = 2
MESH = pl.DeviceIdType.MESH
HI = lax.Precision.HIGHEST
T = 128
NT = (((1,), (1,)), ((), ()))
TN = (((0,), (0,)), ((), ()))
NN = (((1,), (0,)), ((), ()))
DIAGS = ((0, 0), (0, 1), (1, 1))


def dot(a, b, dims=NN):
    return lax.dot_general(a, b, dims, precision=HI, preferred_element_type=jnp.float32)


def factor_tile(aug):
    def strip(i, carry):
        j0 = pl.multiple_of(i * 8, 8)
        rows = aug[pl.ds(j0, 8), :]
        lane = lax.broadcasted_iota(jnp.int32, (8, T), 1)
        sub = lax.broadcasted_iota(jnp.int32, (8, T), 0)
        sub2 = lax.broadcasted_iota(jnp.int32, (8, 2 * T), 0)
        left = rows[:, :T]
        cols = [
            jnp.broadcast_to(
                jnp.sum(jnp.where(lane == j0 + t, left, 0.0), axis=1, keepdims=True), (8, T)
            )
            for t in range(8)
        ]
        for t in range(8):
            p = cols[t][t : t + 1, :]
            r = lax.rsqrt(p)
            r = r * (1.5 - 0.5 * p * r * r)
            coef = cols[t] * r
            for u in range(t + 1, 8):
                head = cols[u][t : t + 1, :] * r
                cols[u] = jnp.where(sub > t, cols[u] - coef * head, cols[u])
            wide_r = jnp.concatenate([r, r], axis=1)
            wide_c = jnp.concatenate([coef, coef], axis=1)
            head = rows[t : t + 1, :] * wide_r
            rows = jnp.where(sub2 == t, head, jnp.where(sub2 > t, rows - wide_c * head, rows))
        aug[pl.ds(j0, 8), :] = rows
        later = jnp.where(lane >= j0 + 8, rows[:, :T], 0.0)
        aug[...] -= dot(later, rows, TN)
        return carry

    lax.fori_loop(0, T // 8, strip, 0)


def split(x):
    top = x.astype(jnp.bfloat16)
    return top, (x - top.astype(jnp.float32)).astype(jnp.bfloat16)


def dot3(left, right, dims=NN):
    acc = None
    for a, b in ((left[1], right[0]), (left[0], right[1]), (left[0], right[0])):
        term = lax.dot_general(a, b, dims, preferred_element_type=jnp.float32)
        acc = term if acc is None else acc + term
    return acc


def kernel(
    shape, first, m_ref, o_ref,
    xs, mbuf, diag, work, aug, w, u01, ufix, cross, y0, y1, z0, bt, top, low,
    dsend, drecv, dloc, xsend, xrecv, csend, crecv, cloc, wsend, wrecv, mload, osend,
):
    n_row, n_col, n_dep = shape
    slots, block, _ = m_ref.shape
    held = slots - first
    half = block // 2
    n_dc = block // T
    n_pair = n_dep // 2
    r = lax.axis_index("row")
    c = lax.axis_index("col")
    d = lax.axis_index("depth")
    j = c * n_dep + d
    sib = d + 1 - 2 * lax.rem(d, 2)
    comm = lax.rem(d, 2) == lax.rem(r, 2)
    chain = jnp.logical_not(comm)
    kr = jnp.minimum(r, PANELS - 1)

    def dest(rr=None, cc=None, dd=None):
        return (r if rr is None else rr, c if cc is None else cc, d if dd is None else dd)

    def remote(src, dst, send, recv, to):
        return pltpu.make_async_remote_copy(
            src_ref=src, dst_ref=dst, send_sem=send, recv_sem=recv,
            device_id=to, device_id_type=MESH,
        )

    def chunks(n):
        if n == 1:
            return [(g * T, 0, block) for g in range(n_dc)]
        out = [(g * T, g * T, block - g * T) for g in range(n_dc)]
        if n == 0:
            out[:1] = [(0, 0, T), (0, T, block - T)]
        return out

    def diag_part(ref, n, g):
        at, col, wide = chunks(n)[g]
        return ref.at[pl.ds(at, T), pl.ds(col, wide)]

    def diag_copy(n, g, lane, to):
        part = diag_part(diag.at[n], n, g)
        return remote(part, part, dsend.at[n, g, lane], drecv.at[n, g], to)

    def diag_load(n, g):
        return pltpu.make_async_copy(
            diag_part(m_ref.at[0], n, g), diag_part(diag.at[n], n, g), dloc.at[n, g]
        )

    def diag_roles(n):
        row, k = DIAGS[n]
        root = (r == row) & (c == 0) & (d == k)
        own_entry = row % 2 == k % 2
        near = d < 2
        entry = comm & near & (c == 0) & (r == row)
        out = [(0, comm & near & (c < n_col - 1), dest(cc=lax.rem(c + 1, n_col)))]
        for q in range(1, n_pair):
            out.append((1 + q, comm & near, dest(dd=lax.rem(sib + 2 * q, n_dep))))
        for step in range(1, n_row):
            rr = lax.rem(r + step, n_row)
            out.append((n_pair + step, entry, dest(rr=rr, dd=lax.rem(rr, 2))))
        down = comm & near
        if not own_entry:
            down = (down & jnp.logical_not(entry)) | root
        out.insert(0, (1, down, dest(dd=sib)))
        rows = [x for x in out if x[0] > n_pair]
        rest = [x for x in out if x[0] <= n_pair]
        return root, rows + rest

    def diag_early(n):
        return DIAGS[n][0] % 2 == DIAGS[n][1] % 2

    def diag_rows(n):
        root, out = diag_roles(n)

        @pl.when(root)
        def _():
            for g in range(len(chunks(n))):
                diag_load(n, g).wait()
                for lane, cond, to in out:
                    if lane > n_pair:
                        diag_copy(n, g, lane, to).start()

    def diag_step(n, g):
        root, out = diag_roles(n)
        early = diag_early(n)

        @pl.when(root)
        def _():
            if not early:
                diag_load(n, g).wait()

        @pl.when(jnp.logical_not(root))
        def _():
            diag_copy(n, g, 0, dest(dd=sib)).wait_recv()

        for lane, cond, to in out:
            if early and lane > n_pair:
                continue

            @pl.when(cond)
            def _():
                diag_copy(n, g, lane, to).start()

    def diag_relay(n):
        for g in range(len(chunks(n))):
            diag_step(n, g)

    def diag_drain(n):
        _, out = diag_roles(n)
        for g in range(len(chunks(n))):
            for lane, cond, to in out:
                @pl.when(cond)
                def _():
                    diag_copy(n, g, lane, to).wait_send()

    def cross_copy(step):
        return remote(
            m_ref.at[0], cross.at[kr], csend.at[step - 1], crecv.at[kr],
            dest(rr=lax.rem(r + step, n_row)),
        )

    def cross_local():
        return pltpu.make_async_copy(m_ref.at[0], cross.at[kr], cloc.at[0])

    def cross_start():
        @pl.when(r < PANELS)
        def _():
            for step in range(1, n_row):
                cross_copy(step).start()

    def cross_wait(k):
        @pl.when(k == r)
        def _():
            cross_local().wait()

        @pl.when(k != r)
        def _():
            remote(
                m_ref.at[0], cross.at[k], csend.at[0], crecv.at[k],
                dest(rr=lax.rem(r + 1, n_row)),
            ).wait_recv()

    def piece(s, side, step):
        cs = c - side * s
        ds = lax.rem(d + 2 * step, n_dep)
        col = jnp.clip(cs, 0, n_col - 1) * n_dep + ds
        a = col // n_row
        ok = comm & (cs >= 0) & (cs < n_col) & (lax.rem(col, n_row) == r) & (a >= first)
        return ok, jnp.clip(a - first, 0, held - 1)

    def along(direction):
        out = []
        for t in range(1, n_col):
            cc = c + direction * t
            lane = (t - 1) if direction > 0 else (n_col - 2 + t)
            out.append((lane, (cc >= 0) & (cc < n_col), dest(cc=jnp.clip(cc, 0, n_col - 1))))
        return out

    def pairs():
        lane = 2 * (n_col - 1)
        return [(lane + q, c >= 0, dest(dd=lax.rem(d + 2 * q, n_dep))) for q in range(1, n_pair)]

    def down():
        return [(2 * (n_col - 1), c >= 0, dest(dd=sib))]

    def piece_out(s, step):
        if step:
            return down()
        return pairs() + down() + (along(-1) + along(1) if s == 0 else [])

    def x_part(k, a, h):
        return xs.at[k, a, pl.ds(pl.multiple_of(h * half, half), half), :]

    def x_copy(k, a, h, lane, to):
        part = x_part(k, a, h)
        return remote(part, part, xsend.at[k, a, h, lane], xrecv.at[k, a, h], to)

    def x_event(s, side, step, k, out=None):
        ok, a = piece(s, side, step)
        lanes = piece_out(s, step) if out is None else out

        @pl.when(ok)
        def _():
            def part(h, carry):
                if s > 0 or step > 0:
                    x_copy(k, a, h, 0, dest(dd=sib)).wait_recv()
                for lane, cond, to in lanes:
                    @pl.when(cond)
                    def _():
                        x_copy(k, a, h, lane, to).start()
                return carry

            lax.fori_loop(0, 2, part, 0)

    places = [(0, 1)] + [(s, side) for s in range(1, n_col) for side in (1, -1)]

    def x_own(k):
        ok, a = piece(0, 1, 0)

        @pl.when(ok)
        def _():
            def turn(e, carry):
                i = pl.multiple_of((e // n_dc) * T, T)
                l = pl.multiple_of(lax.rem(e, n_dc) * T, T)
                xs[k, a, pl.ds(l, T), pl.ds(i, T)] = cross[k, pl.ds(i, T), pl.ds(l, T)].T
                return carry

            lax.fori_loop(0, n_dc * n_dc, turn, 0)

    def x_drain():
        def one(e, carry):
            k = e // 2
            h = lax.rem(e, 2)
            for s, side in places:
                for step in range(n_pair):
                    ok, a = piece(s, side, step)
                    for lane, cond, to in piece_out(s, step):
                        @pl.when(ok & cond)
                        def _():
                            x_copy(k, a, h, lane, to).wait_send()
            return carry

        lax.fori_loop(0, 2 * PANELS, one, 0)

    def w_copy(panel, b):
        rows = pl.ds(pl.multiple_of(b * T, T), T)
        part = w.at[panel, rows, :]
        return remote(part, part, wsend.at[panel, b], wrecv.at[panel, b], dest(dd=sib))

    def u_copy():
        return remote(u01, u01, wsend.at[PANELS, 0], wrecv.at[PANELS, 0], dest(dd=sib))

    def fix_copy():
        return remote(ufix, ufix, wsend.at[PANELS, 1], wrecv.at[PANELS, 1], dest(dd=sib))

    def m_load(s):
        return pltpu.make_async_copy(m_ref.at[s + first], mbuf.at[s + first], mload.at[s])

    def all_loads(wait):
        def one(s, carry):
            if wait:
                m_load(s).wait()
            else:
                m_load(s).start()
            return carry

        lax.fori_loop(0, held, one, 0)

    for n, (row, k) in enumerate(DIAGS):
        @pl.when((d == k) & (c == 0) & (r == row))
        def _():
            for g in range(len(chunks(n))):
                diag_load(n, g).start()

    def eye(rows, columns, at):
        i = lax.broadcasted_iota(jnp.int32, (rows, columns), 0)
        l = lax.broadcasted_iota(jnp.int32, (rows, columns), 1)
        return jnp.where(i + at == l, jnp.float32(1.0), jnp.float32(0.0))

    def upper(x, at):
        i = lax.broadcasted_iota(jnp.int32, x.shape, 0)
        l = lax.broadcasted_iota(jnp.int32, x.shape, 1)
        return jnp.where(i + at <= l, x, 0.0)

    def lower(x, at):
        i = lax.broadcasted_iota(jnp.int32, x.shape, 0)
        l = lax.broadcasted_iota(jnp.int32, x.shape, 1)
        return jnp.where(i + at >= l, x, 0.0)

    def each_tile(f, size=T):
        def step(e, carry):
            f(pl.multiple_of(e * size, size))
            return carry

        lax.fori_loop(0, block // size, step, 0)

    @pl.when(comm)
    def _():
        near = d < 2
        far = jnp.logical_not(near)
        head = near & (c == 0)
        for n in range(len(DIAGS)):
            if diag_early(n):
                diag_rows(n)

        @pl.when(r < PANELS)
        def _():
            cross_local().start()

        source, _ = piece(0, 1, 0)

        def own(kk):
            k = lax.rem(r + kk, PANELS)

            @pl.when(source)
            def _():
                cross_wait(k)
            x_own(k)
            x_event(0, 1, 0, k, down() + along(-1))

        def others(kk):
            x_event(0, 1, 0, lax.rem(r + kk, PANELS), pairs() + along(1))

        @pl.when(jnp.logical_not(head))
        def _():
            own(0)

        @pl.when(far)
        def _():
            others(0)

        @pl.when(near)
        def _():
            for n in range(len(DIAGS)):
                diag_relay(n)

            @pl.when(head)
            def _():
                own(0)
            others(0)

        for kk in range(1, PANELS):
            own(kk)
            others(kk)
        cross_start()

        all_loads(False)
        for kk in range(PANELS):
            k = lax.rem(r + kk, PANELS)
            for s, side in places[1:]:
                x_event(s, side, 0, k)
        for kk in range(PANELS):
            k = lax.rem(r + kk, PANELS)
            for s, side in places:
                for step in range(1, n_pair):
                    x_event(s, side, step, k)
        @pl.when(jnp.logical_not(source))
        def _():
            for k in range(PANELS):
                cross_wait(jnp.int32(k))

        for b in range(n_dc):
            w_copy(0, b).wait_recv()
        u_copy().wait_recv()

    def factor_block(panel):
        def tile(b, carry):
            at = pl.multiple_of(b * T, T)
            rows = pl.ds(at, T)
            aug[:, :T] = work[rows, rows]
            aug[:, T:] = eye(T, T, 0)
            factor_tile(aug)
            if panel == 0:
                @pl.when(b == 0)
                def _():
                    for g in range(1, n_dc + 1):
                        diag_step(0, g)
                    each_tile(fill)
            line = dot(aug[:, T:], work[rows, :])
            work[rows, :] = line
            w[panel, rows, :] = lower(line[:, block:], at)

            @pl.when(r == panel)
            def _():
                ufix[rows, :] = upper(line[:, :block], at)

            @pl.when(b < n_dc - 1)
            def _():
                lane = lax.broadcasted_iota(jnp.int32, (T, block), 1)
                aside = jnp.where(lane >= at + T, line[:, :block], 0.0)

                def tail(e, carry2):
                    cols = pl.ds(pl.multiple_of(e * 2 * T, 2 * T), 2 * T)
                    work[:, cols] -= dot(aside, work[rows, cols], TN)
                    return carry2

                lax.fori_loop(0, block // T, tail, 0)

            w_copy(panel, b).start()
            return carry

        lax.fori_loop(0, n_dc, tile, 0)

    def fill(at):
        rows = pl.ds(at, T)
        work[rows, :block] = diag[0, rows, :]
        work[rows, block:] = eye(T, block, at)

    def join(at):
        rows = pl.ds(at, T)
        u01[rows, :] = dot(w[0, rows, :], diag[1])

    def second(at):
        rows = pl.ds(at, T)
        work[rows, :block] = diag[2, rows, :] - dot(u01[:, rows], u01[...], TN)
        work[rows, block:] = eye(T, block, at)

    @pl.when(chain)
    def _():
        head = (d < 2) & (c == 0)

        @pl.when(r < PANELS)
        def _():
            cross_local().start()

        @pl.when(jnp.logical_not(head))
        def _():
            cross_start()

        diag_step(0, 0)
        work[pl.ds(0, T), pl.ds(0, T)] = diag[0, pl.ds(0, T), pl.ds(0, T)]
        all_loads(False)
        diag_start = DIAGS[1]

        @pl.when((r == diag_start[0]) & (c == 0) & (d == diag_start[1]))
        def _():
            diag_relay(1)

        factor_block(0)

        @pl.when(head)
        def _():
            cross_start()

        @pl.when(jnp.logical_not((r == diag_start[0]) & (c == 0) & (d == diag_start[1])))
        def _():
            diag_relay(1)

        each_tile(join)
        u_copy().start()
        diag_relay(2)
        each_tile(second)
        factor_block(1)
        for k in range(PANELS):
            cross_wait(jnp.int32(k))

        @pl.when(r < PANELS)
        def _():
            fix_copy().start()

    def unit(k, x, at):
        i1 = lax.broadcasted_iota(jnp.int32, x.shape, 0)
        i2 = lax.broadcasted_iota(jnp.int32, x.shape, 1)
        minus = jnp.where((i1 + at == i2) & (j == k), jnp.float32(-1.0), 0.0)
        return jnp.where(j < PANELS, minus, x)

    def cut(ref, *index):
        return split(ref[index])

    def s1(at):
        rows = pl.ds(at, half)
        y0[rows, :] = unit(0, dot3(split(w[0, rows, :]), split(cross[0])), at)

    def s2(at):
        rows = pl.ds(at, half)
        y1[rows, :] = cross[1, rows, :] - dot3(split(u01[:, rows]), split(y0[...]), TN)

    def s3(at):
        rows = pl.ds(at, half)
        z0[rows, :] = dot3(split(w[0, :, rows]), split(y0[...]), TN)
        bt[rows, :] = dot3(split(w[0, :, rows]), split(u01[...]), TN)

    def s4(at):
        rows = pl.ds(at, half)
        y0[rows, :] = unit(1, dot3(split(w[1, rows, :]), split(y1[...])), at)

    def s5(at):
        rows = pl.ds(at, half)
        value = dot3(split(w[1, :, rows]), split(y0[...]), TN)
        top[1, rows, :], low[1, rows, :] = split(value)

    def s6(at):
        rows = pl.ds(at, half)
        value = z0[rows, :] - dot3(split(bt[rows, :]), (top[1], low[1]))
        top[0, rows, :], low[0, rows, :] = split(value)

    each_tile(s1, half)
    each_tile(s2, half)
    each_tile(s3, half)

    @pl.when(comm)
    def _():
        for b in range(n_dc):
            w_copy(1, b).wait_recv()

    each_tile(s4, half)
    each_tile(s5, half)
    each_tile(s6, half)

    @pl.when(chain)
    def _():
        def arrive(e, carry):
            x_copy(e // (2 * held), lax.rem(e // 2, held), lax.rem(e, 2), 0, dest(dd=sib)).wait_recv()
            return carry

        lax.fori_loop(0, PANELS * held * 2, arrive, 0)

    all_loads(True)

    def out_copy(s, h):
        rows = pl.ds(pl.multiple_of(h * half, half), half)
        return pltpu.make_async_copy(mbuf.at[s, rows, :], o_ref.at[s, rows, :], osend.at[s, h])

    def update(e, carry):
        a = e // 2
        h = lax.rem(e, 2)
        rows = pl.ds(pl.multiple_of(h * half, half), half)
        acc = jnp.where(j >= PANELS, mbuf[a + first, rows, :], 0.0)
        for k in range(PANELS):
            acc = acc - dot3(split(xs[k, a, rows, :]), (top[k], low[k]))
        mbuf[a + first, rows, :] = acc
        if first:
            out_copy(a + first, h).start()
        else:
            @pl.when((a > 0) | (r >= PANELS))
            def _():
                out_copy(a, h).start()
        return carry

    lax.fori_loop(0, 2 * held, update, 0)

    @pl.when(r < PANELS)
    def _():
        @pl.when(comm)
        def _():
            fix_copy().wait_recv()

        mbuf[0] = jnp.zeros((block, block), jnp.float32)

        def turned(ref):
            def turn(e, carry):
                i = pl.multiple_of((e // n_dc) * T, T)
                l = pl.multiple_of(lax.rem(e, n_dc) * T, T)
                mbuf[0, pl.ds(l, T), pl.ds(i, T)] = ref[pl.ds(i, T), pl.ds(l, T)].T
                return carry

            lax.fori_loop(0, n_dc * n_dc, turn, 0)

        @pl.when(j == r)
        def _():
            turned(ufix)

        @pl.when((j == 0) & (r == 1))
        def _():
            turned(u01)

        for h in range(2):
            out_copy(0, h).start()

    if first:
        pass

    @pl.when(r < PANELS)
    def _():
        for step in range(1, n_row):
            cross_copy(step).wait_send()

    @pl.when(chain)
    def _():
        for panel in range(PANELS):
            for b in range(n_dc):
                w_copy(panel, b).wait_send()
        u_copy().wait_send()

        @pl.when(r < PANELS)
        def _():
            fix_copy().wait_send()

    for n in range(len(DIAGS)):
        diag_drain(n)
    x_drain()

    def finish(e, carry):
        out_copy(e // 2, lax.rem(e, 2)).wait()
        return carry

    lax.fori_loop(0, 2 * slots, finish, 0)


def body(shape, matrix):
    n_row, n_col, n_dep = shape
    m = matrix.reshape(matrix.shape[0], matrix.shape[2], matrix.shape[3])
    slots, block, _ = m.shape
    first = 1 if n_row <= PANELS else 0
    held = slots - first
    n_dc = block // T
    n_pair = n_dep // 2
    f32 = jnp.float32
    dma = pltpu.SemaphoreType.DMA
    hbm = pl.BlockSpec(memory_space=pltpu.HBM)
    square = pltpu.VMEM((block, block), f32)
    out = pl.pallas_call(
        functools.partial(kernel, shape, first),
        out_shape=jax.ShapeDtypeStruct(m.shape, f32),
        in_specs=[hbm],
        out_specs=hbm,
        scratch_shapes=[
            pltpu.VMEM((PANELS, held, block, block), f32),
            pltpu.VMEM((slots, block, block), f32),
            pltpu.VMEM((len(DIAGS), block, block), f32),
            pltpu.VMEM((block, 2 * block), f32),
            pltpu.VMEM((T, 2 * T), f32),
            pltpu.VMEM((PANELS, block, block), f32),
            square, square,
            pltpu.VMEM((PANELS, block, block), f32),
            square, square, square, square,
            pltpu.VMEM((PANELS, block, block), jnp.bfloat16),
            pltpu.VMEM((PANELS, block, block), jnp.bfloat16),
            dma((len(DIAGS), n_dc + 1, n_pair + n_row)),
            dma((len(DIAGS), n_dc + 1)),
            dma((len(DIAGS), n_dc + 1)),
            dma((PANELS, held, 2, 2 * (n_col - 1) + n_pair)),
            dma((PANELS, held, 2)),
            dma((n_row - 1,)),
            dma((PANELS,)),
            dma((1,)),
            dma((PANELS + 1, n_dc)),
            dma((PANELS + 1, n_dc)),
            dma((held,)),
            dma((slots, 2)),
        ],
        compiler_params=pltpu.CompilerParams(has_side_effects=True, vmem_limit_bytes=60 << 20),
    )(m)
    return out.reshape(matrix.shape)


def solution(mesh):
    shape = (mesh.shape["row"], mesh.shape["col"], mesh.shape["depth"])
    placed = P(None, "row", None, ("col", "depth"))
    return jax.shard_map(
        functools.partial(body, shape),
        mesh=mesh,
        in_specs=(placed,),
        out_specs=placed,
        check_vma=False,
    )
```

```python
import functools

import jax
import jax.numpy as jnp
from jax import lax
from jax.experimental import pallas as pl
from jax.experimental.pallas import tpu as pltpu
from jax.sharding import PartitionSpec as P

PANELS = 2
MESH = pl.DeviceIdType.MESH
HI = lax.Precision.HIGHEST
T = 128
S = 16
H = 4
NT = (((1,), (1,)), ((), ()))
TN = (((0,), (0,)), ((), ()))
NN = (((1,), (0,)), ((), ()))
DIAGS = ((0, 0), (0, 1), (1, 1))


def dot(a, b, dims=NN):
    return lax.dot_general(a, b, dims, precision=HI, preferred_element_type=jnp.float32)


def stacked(x, order, axis):
    top = x.astype(jnp.bfloat16)
    rest = x - top.astype(jnp.float32)
    mid = rest.astype(jnp.bfloat16)
    low = (rest - mid.astype(jnp.float32)).astype(jnp.bfloat16)
    parts = (top, mid, low)
    return jnp.concatenate([parts[i] for i in order], axis=axis)


def left6(x, axis):
    return stacked(x, (1, 2, 0, 1, 0, 0), axis)


def right6(x, axis=0):
    return stacked(x, (1, 0, 2, 0, 1, 0), axis)


def dot6(left, right, dims=NN):
    return lax.dot_general(left, right, dims, preferred_element_type=jnp.float32)


def factor_tile(aug):
    n_part = S // 8

    def strip(i, carry):
        j0 = pl.multiple_of(i * S, S)
        rows = [aug[pl.ds(j0 + 8 * p, 8), :] for p in range(n_part)]
        lane = lax.broadcasted_iota(jnp.int32, (8, T), 1)
        sub = lax.broadcasted_iota(jnp.int32, (8, T), 0)
        sub2 = lax.broadcasted_iota(jnp.int32, (8, 2 * T), 0)
        cols = [
            [
                jnp.broadcast_to(
                    jnp.sum(jnp.where(lane == j0 + t, x[:, :T], 0.0), axis=1, keepdims=True), (8, T)
                )
                for t in range(S)
            ]
            for x in rows
        ]
        for t in range(S):
            q, e = t // 8, t % 8
            p = cols[q][t][e : e + 1, :]
            r = lax.rsqrt(p)
            r = r * (1.5 - 0.5 * p * r * r)
            coef = {g: cols[g][t] * r for g in range(q, n_part)}
            for u in range(t + 1, S):
                head = cols[q][u][e : e + 1, :] * r
                cols[q][u] = jnp.where(sub > e, cols[q][u] - coef[q] * head, cols[q][u])
                for g in range(q + 1, n_part):
                    cols[g][u] = cols[g][u] - coef[g] * head
            wide_r = jnp.concatenate([r, r], axis=1)
            head = rows[q][e : e + 1, :] * wide_r
            wide_c = jnp.concatenate([coef[q], coef[q]], axis=1)
            rows[q] = jnp.where(
                sub2 == e, head, jnp.where(sub2 > e, rows[q] - wide_c * head, rows[q])
            )
            for g in range(q + 1, n_part):
                wide_c = jnp.concatenate([coef[g], coef[g]], axis=1)
                rows[g] = rows[g] - wide_c * head
        done = jnp.concatenate(rows, axis=0)
        aug[pl.ds(j0, S), :] = done
        wide = lax.broadcasted_iota(jnp.int32, (S, T), 1)
        later = jnp.where(wide >= j0 + S, done[:, :T], 0.0)
        aug[...] -= dot6(left6(later, 0), right6(done), TN)
        return carry

    lax.fori_loop(0, T // S, strip, 0)


def split(x):
    top = x.astype(jnp.bfloat16)
    return top, (x - top.astype(jnp.float32)).astype(jnp.bfloat16)


def dot3(left, right, dims=NN):
    acc = None
    for a, b in ((left[1], right[0]), (left[0], right[1]), (left[0], right[0])):
        term = lax.dot_general(a, b, dims, preferred_element_type=jnp.float32)
        acc = term if acc is None else acc + term
    return acc


def kernel(
    shape, first, m_ref, o_ref,
    xs, mbuf, diag, work, aug, w, u01, ufix, cross, y0, y1, z0, bt, top, low,
    dsend, drecv, dloc, xsend, xrecv, csend, crecv, cloc, wsend, wrecv, mload, osend,
):
    n_row, n_col, n_dep = shape
    slots, block, _ = m_ref.shape
    held = slots - first
    half = block // 2
    n_dc = block // T
    n_pair = n_dep // 2
    r = lax.axis_index("row")
    c = lax.axis_index("col")
    d = lax.axis_index("depth")
    j = c * n_dep + d
    sib = d + 1 - 2 * lax.rem(d, 2)
    comm = lax.rem(d, 2) == lax.rem(r, 2)
    chain = jnp.logical_not(comm)
    kr = jnp.minimum(r, PANELS - 1)

    def dest(rr=None, cc=None, dd=None):
        return (r if rr is None else rr, c if cc is None else cc, d if dd is None else dd)

    def remote(src, dst, send, recv, to):
        return pltpu.make_async_remote_copy(
            src_ref=src, dst_ref=dst, send_sem=send, recv_sem=recv,
            device_id=to, device_id_type=MESH,
        )

    def chunks(n):
        if n == 1:
            return [(g * T, 0, block) for g in range(n_dc)]
        out = [(g * T, g * T, block - g * T) for g in range(n_dc)]
        if n == 0:
            out[:1] = [(0, 0, T), (0, T, block - T)]
        return out

    def diag_part(ref, n, g):
        at, col, wide = chunks(n)[g]
        return ref.at[pl.ds(at, T), pl.ds(col, wide)]

    def diag_copy(n, g, lane, to):
        part = diag_part(diag.at[n], n, g)
        return remote(part, part, dsend.at[n, g, lane], drecv.at[n, g], to)

    def diag_load(n, g):
        return pltpu.make_async_copy(
            diag_part(m_ref.at[0], n, g), diag_part(diag.at[n], n, g), dloc.at[n, g]
        )

    def diag_roles(n):
        row, k = DIAGS[n]
        root = (r == row) & (c == 0) & (d == k)
        own_entry = row % 2 == k % 2
        near = d < 2
        entry = comm & near & (c == 0) & (r == row)
        out = [(0, comm & near & (c < n_col - 1), dest(cc=lax.rem(c + 1, n_col)))]
        for q in range(1, n_pair):
            out.append((1 + q, comm & near, dest(dd=lax.rem(sib + 2 * q, n_dep))))
        for step in range(1, n_row):
            rr = lax.rem(r + step, n_row)
            out.append((n_pair + step, entry, dest(rr=rr, dd=lax.rem(rr, 2))))
        down = comm & near
        if not own_entry:
            down = (down & jnp.logical_not(entry)) | root
        out.insert(0, (1, down, dest(dd=sib)))
        rows = [x for x in out if x[0] > n_pair]
        rest = [x for x in out if x[0] <= n_pair]
        return root, rows + rest

    def diag_early(n):
        return DIAGS[n][0] % 2 == DIAGS[n][1] % 2

    def diag_rows(n):
        root, out = diag_roles(n)

        @pl.when(root)
        def _():
            for g in range(len(chunks(n))):
                diag_load(n, g).wait()
                for lane, cond, to in out:
                    if lane > n_pair:
                        diag_copy(n, g, lane, to).start()

    def diag_step(n, g):
        root, out = diag_roles(n)
        early = diag_early(n)

        @pl.when(root)
        def _():
            if not early:
                diag_load(n, g).wait()

        @pl.when(jnp.logical_not(root))
        def _():
            diag_copy(n, g, 0, dest(dd=sib)).wait_recv()

        for lane, cond, to in out:
            if early and lane > n_pair:
                continue

            @pl.when(cond)
            def _():
                diag_copy(n, g, lane, to).start()

    def diag_relay(n):
        for g in range(len(chunks(n))):
            diag_step(n, g)

    def diag_drain(n):
        _, out = diag_roles(n)
        for g in range(len(chunks(n))):
            for lane, cond, to in out:
                @pl.when(cond)
                def _():
                    diag_copy(n, g, lane, to).wait_send()

    def cross_copy(step):
        return remote(
            m_ref.at[0], cross.at[kr], csend.at[step - 1], crecv.at[kr],
            dest(rr=lax.rem(r + step, n_row)),
        )

    def cross_local():
        return pltpu.make_async_copy(m_ref.at[0], cross.at[kr], cloc.at[0])

    def cross_start():
        @pl.when(r < PANELS)
        def _():
            for step in range(1, n_row):
                cross_copy(step).start()

    def cross_wait(k):
        @pl.when(k == r)
        def _():
            cross_local().wait()

        @pl.when(k != r)
        def _():
            remote(
                m_ref.at[0], cross.at[k], csend.at[0], crecv.at[k],
                dest(rr=lax.rem(r + 1, n_row)),
            ).wait_recv()

    def piece(s, side, step):
        cs = c - side * s
        ds = lax.rem(d + 2 * step, n_dep)
        col = jnp.clip(cs, 0, n_col - 1) * n_dep + ds
        a = col // n_row
        ok = comm & (cs >= 0) & (cs < n_col) & (lax.rem(col, n_row) == r) & (a >= first)
        return ok, jnp.clip(a - first, 0, held - 1)

    def along(direction):
        out = []
        for t in range(1, n_col):
            cc = c + direction * t
            lane = (t - 1) if direction > 0 else (n_col - 2 + t)
            out.append((lane, (cc >= 0) & (cc < n_col), dest(cc=jnp.clip(cc, 0, n_col - 1))))
        return out

    def pairs():
        lane = 2 * (n_col - 1)
        return [(lane + q, c >= 0, dest(dd=lax.rem(d + 2 * q, n_dep))) for q in range(1, n_pair)]

    def down():
        return [(2 * (n_col - 1), c >= 0, dest(dd=sib))]

    def piece_out(s, step):
        if step:
            return down()
        return pairs() + down() + (along(-1) + along(1) if s == 0 else [])

    def x_part(k, a, h):
        size = block // H
        return xs.at[k, a, pl.ds(pl.multiple_of(h * size, size), size), :]

    def x_copy(k, a, h, lane, to):
        part = x_part(k, a, h)
        return remote(part, part, xsend.at[k, a, h, lane], xrecv.at[k, a, h], to)

    def x_send(k, out):
        ok, a = piece(0, 1, 0)

        @pl.when(ok)
        def _():
            def part(h, carry):
                for lane, cond, to in out:
                    @pl.when(cond)
                    def _():
                        x_copy(k, a, h, lane, to).start()
                return carry

            lax.fori_loop(0, H, part, 0)

    def x_event(s, side, step, k, h):
        ok, a = piece(s, side, step)

        @pl.when(ok)
        def _():
            x_copy(k, a, h, 0, dest(dd=sib)).wait_recv()
            for lane, cond, to in piece_out(s, step):
                x_copy(k, a, h, lane, to).start()

    def turn_of(e):
        return lax.rem(r + e // H, PANELS), lax.rem(e, H)

    def x_line(e):
        k, h = turn_of(e)
        for s, side in places[1:]:
            x_event(s, side, 0, k, h)

    def x_across(e):
        k, h = turn_of(e)
        for s, side in places:
            for step in range(1, n_pair):
                x_event(s, side, step, k, h)

    places = [(0, 1)] + [(s, side) for s in range(1, n_col) for side in (1, -1)]

    def x_own(k):
        ok, a = piece(0, 1, 0)

        @pl.when(ok)
        def _():
            def turn(e, carry):
                i = pl.multiple_of((e // n_dc) * T, T)
                l = pl.multiple_of(lax.rem(e, n_dc) * T, T)
                xs[k, a, pl.ds(l, T), pl.ds(i, T)] = cross[k, pl.ds(i, T), pl.ds(l, T)].T
                return carry

            lax.fori_loop(0, n_dc * n_dc, turn, 0)

    def x_drain():
        def one(e, carry):
            k = e // H
            h = lax.rem(e, H)
            for s, side in places:
                for step in range(n_pair):
                    ok, a = piece(s, side, step)
                    for lane, cond, to in piece_out(s, step):
                        @pl.when(ok & cond)
                        def _():
                            x_copy(k, a, h, lane, to).wait_send()
            return carry

        lax.fori_loop(0, H * PANELS, one, 0)

    def w_copy(panel, b):
        rows = pl.ds(pl.multiple_of(b * T, T), T)
        part = w.at[panel, rows, :]
        return remote(part, part, wsend.at[panel, b], wrecv.at[panel, b], dest(dd=sib))

    def u_copy():
        return remote(u01, u01, wsend.at[PANELS, 0], wrecv.at[PANELS, 0], dest(dd=sib))

    def fix_copy():
        return remote(ufix, ufix, wsend.at[PANELS, 1], wrecv.at[PANELS, 1], dest(dd=sib))

    def m_load(s):
        return pltpu.make_async_copy(m_ref.at[s + first], mbuf.at[s + first], mload.at[s])

    def all_loads(wait):
        def one(s, carry):
            if wait:
                m_load(s).wait()
            else:
                m_load(s).start()
            return carry

        lax.fori_loop(0, held, one, 0)

    for n, (row, k) in enumerate(DIAGS):
        @pl.when((d == k) & (c == 0) & (r == row))
        def _():
            for g in range(len(chunks(n))):
                diag_load(n, g).start()

    def eye(rows, columns, at):
        i = lax.broadcasted_iota(jnp.int32, (rows, columns), 0)
        l = lax.broadcasted_iota(jnp.int32, (rows, columns), 1)
        return jnp.where(i + at == l, jnp.float32(1.0), jnp.float32(0.0))

    def upper(x, at):
        i = lax.broadcasted_iota(jnp.int32, x.shape, 0)
        l = lax.broadcasted_iota(jnp.int32, x.shape, 1)
        return jnp.where(i + at <= l, x, 0.0)

    def lower(x, at):
        i = lax.broadcasted_iota(jnp.int32, x.shape, 0)
        l = lax.broadcasted_iota(jnp.int32, x.shape, 1)
        return jnp.where(i + at >= l, x, 0.0)

    def each_tile(f, size=T):
        def step(e, carry):
            f(pl.multiple_of(e * size, size))
            return carry

        lax.fori_loop(0, block // size, step, 0)

    def unit(k, x, at):
        i1 = lax.broadcasted_iota(jnp.int32, x.shape, 0)
        i2 = lax.broadcasted_iota(jnp.int32, x.shape, 1)
        minus = jnp.where((i1 + at == i2) & (j == k), jnp.float32(-1.0), 0.0)
        return jnp.where(j < PANELS, minus, x)

    def cut(ref, *index):
        return split(ref[index])

    def s1(at):
        rows = pl.ds(at, half)
        y0[rows, :] = unit(0, dot3(split(w[0, rows, :]), split(cross[0])), at)

    def s2(at):
        rows = pl.ds(at, half)
        y1[rows, :] = cross[1, rows, :] - dot3(split(u01[:, rows]), split(y0[...]), TN)

    def s3(at):
        rows = pl.ds(at, half)
        z0[rows, :] = dot3(split(w[0, :, rows]), split(y0[...]), TN)
        bt[rows, :] = dot3(split(w[0, :, rows]), split(u01[...]), TN)

    def early():
        each_tile(s1, half)
        each_tile(s2, half)
        each_tile(s3, half)

    def s4(at):
        rows = pl.ds(at, half)
        y0[rows, :] = unit(1, dot3(split(w[1, rows, :]), split(y1[...])), at)

    def s5(at):
        rows = pl.ds(at, half)
        value = dot3(split(w[1, :, rows]), split(y0[...]), TN)
        top[1, rows, :], low[1, rows, :] = split(value)

    def s6(at):
        rows = pl.ds(at, half)
        value = z0[rows, :] - dot3(split(bt[rows, :]), (top[1], low[1]))
        top[0, rows, :], low[0, rows, :] = split(value)

    def middle():
        each_tile(s4, half)
        each_tile(s5, half)
        each_tile(s6, half)

    def out_copy(s, h):
        rows = pl.ds(pl.multiple_of(h * (block // H), block // H), block // H)
        return pltpu.make_async_copy(mbuf.at[s, rows, :], o_ref.at[s, rows, :], osend.at[s, h])

    def update(h):
        rows = pl.ds(pl.multiple_of(h * (block // H), block // H), block // H)

        def one(a, carry):
            acc = jnp.where(j >= PANELS, mbuf[a + first, rows, :], 0.0)
            for k in range(PANELS):
                acc = acc - dot3(split(xs[k, a, rows, :]), (top[k], low[k]))
            if first:
                mbuf[a + first, rows, :] = acc
                out_copy(a + first, h).start()
            else:
                @pl.when((a > 0) | (r >= PANELS))
                def _():
                    mbuf[a, rows, :] = acc
                    out_copy(a, h).start()
            return carry

        lax.fori_loop(0, held, one, 0)

    def rest_of_update():
        def one(h, carry):
            update(h)
            return carry

        lax.fori_loop(2, H, one, 0)

    def corner():
        def turned(ref):
            def turn(e, carry):
                i = pl.multiple_of((e // n_dc) * T, T)
                l = pl.multiple_of(lax.rem(e, n_dc) * T, T)
                mbuf[0, pl.ds(l, T), pl.ds(i, T)] = ref[pl.ds(i, T), pl.ds(l, T)].T
                return carry

            lax.fori_loop(0, n_dc * n_dc, turn, 0)

        @pl.when(r < PANELS)
        def _():
            @pl.when(comm)
            def _():
                fix_copy().wait_recv()

            mbuf[0] = jnp.zeros((block, block), jnp.float32)

            @pl.when(j == r)
            def _():
                turned(ufix)

            @pl.when((j == 0) & (r == 1))
            def _():
                turned(u01)

            for h in range(H):
                out_copy(0, h).start()

    @pl.when(comm)
    def _():
        near = d < 2
        far = jnp.logical_not(near)
        head = near & (c == 0)
        for n in range(len(DIAGS)):
            if diag_early(n):
                diag_rows(n)

        @pl.when(r < PANELS)
        def _():
            cross_local().start()

        source, _ = piece(0, 1, 0)

        def own(kk):
            k = lax.rem(r + kk, PANELS)

            @pl.when(source)
            def _():
                cross_wait(k)
            x_own(k)
            x_send(k, down() + along(-1))

        def others(kk):
            x_send(lax.rem(r + kk, PANELS), pairs() + along(1))

        @pl.when(jnp.logical_not(head))
        def _():
            own(0)

        @pl.when(far)
        def _():
            others(0)

        @pl.when(near)
        def _():
            for n in range(len(DIAGS)):
                diag_relay(n)

            @pl.when(head)
            def _():
                own(0)
            others(0)

        for kk in range(1, PANELS):
            own(kk)
            others(kk)
        cross_start()

        all_loads(False)
        n_event = PANELS * H
        lead = n_event // 2

        def first_part(e, carry):
            x_line(e)
            return carry

        def second_part(e, carry):
            @pl.when(e == lead // 2)
            def _():
                @pl.when(jnp.logical_not(source))
                def _():
                    for k in range(PANELS):
                        cross_wait(jnp.int32(k))

                for b in range(n_dc):
                    w_copy(0, b).wait_recv()
                u_copy().wait_recv()
                early()

            x_line(lead + e)

            @pl.when(e > 0)
            def _():
                x_across(2 * e - 1)
            x_across(2 * e)
            return carry

        lax.fori_loop(0, lead, first_part, 0)
        lax.fori_loop(0, lead, second_part, 0)
        for b in range(n_dc):
            w_copy(1, b).wait_recv()
        middle()
        all_loads(True)
        corner()
        update(0)
        update(1)
        x_across(n_event - 1)
        rest_of_update()

    def factor_block(panel):
        def tile(b, carry):
            at = pl.multiple_of(b * T, T)
            rows = pl.ds(at, T)
            aug[:, :T] = work[rows, rows]
            aug[:, T:] = eye(T, T, 0)
            factor_tile(aug)
            if panel == 0:
                @pl.when(b == 0)
                def _():
                    for g in range(1, n_dc + 1):
                        diag_step(0, g)
                    each_tile(fill)
            line = dot6(left6(aug[:, T:], 1), right6(work[rows, :]))
            work[rows, :] = line
            w[panel, rows, :] = lower(line[:, block:], at)

            @pl.when(r == panel)
            def _():
                ufix[rows, :] = upper(line[:, :block], at)

            @pl.when(b < n_dc - 1)
            def _():
                lane = lax.broadcasted_iota(jnp.int32, (T, block), 1)
                aside = jnp.where(lane >= at + T, line[:, :block], 0.0)

                left = left6(aside, 0)

                def tail(e, carry2):
                    cols = pl.ds(pl.multiple_of(e * 2 * T, 2 * T), 2 * T)
                    work[:, cols] -= dot6(left, right6(work[rows, cols]), TN)
                    return carry2

                lax.fori_loop((b + 1) // 2, block // (2 * T) + b // 2 + 1, tail, 0)

            w_copy(panel, b).start()
            return carry

        lax.fori_loop(0, n_dc, tile, 0)

    def fill(at):
        rows = pl.ds(at, T)
        work[rows, :block] = diag[0, rows, :]
        work[rows, block:] = eye(T, block, at)

    def join(at):
        rows = pl.ds(at, T)
        u01[rows, :] = dot(w[0, rows, :], diag[1])

    def second(at):
        rows = pl.ds(at, T)
        work[rows, :block] = diag[2, rows, :] - dot(u01[:, rows], u01[...], TN)
        work[rows, block:] = eye(T, block, at)

    @pl.when(chain)
    def _():
        head = (d < 2) & (c == 0)

        @pl.when(r < PANELS)
        def _():
            cross_local().start()

        @pl.when(jnp.logical_not(head))
        def _():
            cross_start()

        diag_step(0, 0)
        work[pl.ds(0, T), pl.ds(0, T)] = diag[0, pl.ds(0, T), pl.ds(0, T)]
        all_loads(False)
        diag_start = DIAGS[1]

        @pl.when((r == diag_start[0]) & (c == 0) & (d == diag_start[1]))
        def _():
            diag_relay(1)

        factor_block(0)

        @pl.when(head)
        def _():
            cross_start()

        @pl.when(jnp.logical_not((r == diag_start[0]) & (c == 0) & (d == diag_start[1])))
        def _():
            diag_relay(1)

        each_tile(join)
        u_copy().start()
        diag_relay(2)
        each_tile(second)
        factor_block(1)
        for k in range(PANELS):
            cross_wait(jnp.int32(k))

        @pl.when(r < PANELS)
        def _():
            fix_copy().start()

        early()
        middle()
        all_loads(True)
        corner()

        def last(h, carry):
            def arrive(e, carry2):
                x_copy(e // held, lax.rem(e, held), h, 0, dest(dd=sib)).wait_recv()
                return carry2

            lax.fori_loop(0, PANELS * held, arrive, 0)
            update(h)
            return carry

        lax.fori_loop(0, H, last, 0)

    @pl.when(r < PANELS)
    def _():
        for step in range(1, n_row):
            cross_copy(step).wait_send()

    @pl.when(chain)
    def _():
        for panel in range(PANELS):
            for b in range(n_dc):
                w_copy(panel, b).wait_send()
        u_copy().wait_send()

        @pl.when(r < PANELS)
        def _():
            fix_copy().wait_send()

    for n in range(len(DIAGS)):
        diag_drain(n)
    x_drain()

    def finish(e, carry):
        out_copy(e // H, lax.rem(e, H)).wait()
        return carry

    lax.fori_loop(0, H * slots, finish, 0)


def body(shape, matrix):
    n_row, n_col, n_dep = shape
    m = matrix.reshape(matrix.shape[0], matrix.shape[2], matrix.shape[3])
    slots, block, _ = m.shape
    first = 1 if n_row <= PANELS else 0
    held = slots - first
    n_dc = block // T
    n_pair = n_dep // 2
    f32 = jnp.float32
    dma = pltpu.SemaphoreType.DMA
    hbm = pl.BlockSpec(memory_space=pltpu.HBM)
    square = pltpu.VMEM((block, block), f32)
    out = pl.pallas_call(
        functools.partial(kernel, shape, first),
        out_shape=jax.ShapeDtypeStruct(m.shape, f32),
        in_specs=[hbm],
        out_specs=pl.BlockSpec(memory_space=pl.ANY),
        scratch_shapes=[
            pltpu.VMEM((PANELS, held, block, block), f32),
            pltpu.VMEM((slots, block, block), f32),
            pltpu.VMEM((len(DIAGS), block, block), f32),
            pltpu.VMEM((block, 2 * block), f32),
            pltpu.VMEM((T, 2 * T), f32),
            pltpu.VMEM((PANELS, block, block), f32),
            square, square,
            pltpu.VMEM((PANELS, block, block), f32),
            square, square, square, square,
            pltpu.VMEM((PANELS, block, block), jnp.bfloat16),
            pltpu.VMEM((PANELS, block, block), jnp.bfloat16),
            dma((len(DIAGS), n_dc + 1, n_pair + n_row)),
            dma((len(DIAGS), n_dc + 1)),
            dma((len(DIAGS), n_dc + 1)),
            dma((PANELS, held, H, 2 * (n_col - 1) + n_pair)),
            dma((PANELS, held, H)),
            dma((n_row - 1,)),
            dma((PANELS,)),
            dma((1,)),
            dma((PANELS + 1, n_dc)),
            dma((PANELS + 1, n_dc)),
            dma((held,)),
            dma((slots, H)),
        ],
        compiler_params=pltpu.CompilerParams(has_side_effects=True, vmem_limit_bytes=44 << 20),
    )(m)
    return out.reshape(matrix.shape)


def solution(mesh):
    shape = (mesh.shape["row"], mesh.shape["col"], mesh.shape["depth"])
    placed = P(None, "row", None, ("col", "depth"))
    return jax.shard_map(
        functools.partial(body, shape),
        mesh=mesh,
        in_specs=(placed,),
        out_specs=placed,
        check_vma=False,
    )
```

```python
import functools

import jax
import jax.numpy as jnp
from jax import lax
from jax.experimental import pallas as pl
from jax.experimental.pallas import tpu as pltpu
from jax.sharding import PartitionSpec as P

PANELS = 2
MESH = pl.DeviceIdType.MESH
HI = lax.Precision.HIGHEST
T = 128
S = 16
H = 4
NT = (((1,), (1,)), ((), ()))
TN = (((0,), (0,)), ((), ()))
NN = (((1,), (0,)), ((), ()))
DIAGS = ((0, 0), (0, 1), (1, 1))


def dot(a, b, dims=NN):
    return lax.dot_general(a, b, dims, precision=HI, preferred_element_type=jnp.float32)


def stacked(x, order, axis):
    top = x.astype(jnp.bfloat16)
    rest = x - top.astype(jnp.float32)
    mid = rest.astype(jnp.bfloat16)
    low = (rest - mid.astype(jnp.float32)).astype(jnp.bfloat16)
    parts = (top, mid, low)
    return jnp.concatenate([parts[i] for i in order], axis=axis)


def left6(x, axis):
    return stacked(x, (1, 2, 0, 1, 0, 0), axis)


def right6(x, axis=0):
    return stacked(x, (1, 0, 2, 0, 1, 0), axis)


def dot6(left, right, dims=NN):
    return lax.dot_general(left, right, dims, preferred_element_type=jnp.float32)


def factor_tile(aug):
    n_part = S // 8

    def strip(i, carry):
        j0 = pl.multiple_of(i * S, S)
        rows = [aug[pl.ds(j0 + 8 * p, 8), :] for p in range(n_part)]
        lane = lax.broadcasted_iota(jnp.int32, (8, T), 1)
        sub = lax.broadcasted_iota(jnp.int32, (8, T), 0)
        sub2 = lax.broadcasted_iota(jnp.int32, (8, 2 * T), 0)
        cols = [
            [
                jnp.broadcast_to(
                    jnp.sum(jnp.where(lane == j0 + t, x[:, :T], 0.0), axis=1, keepdims=True), (8, T)
                )
                for t in range(S)
            ]
            for x in rows
        ]
        for t in range(S):
            q, e = t // 8, t % 8
            p = cols[q][t][e : e + 1, :]
            r = lax.rsqrt(p)
            r = r * (1.5 - 0.5 * p * r * r)
            coef = {g: cols[g][t] * r for g in range(q, n_part)}
            for u in range(t + 1, S):
                head = cols[q][u][e : e + 1, :] * r
                cols[q][u] = jnp.where(sub > e, cols[q][u] - coef[q] * head, cols[q][u])
                for g in range(q + 1, n_part):
                    cols[g][u] = cols[g][u] - coef[g] * head
            wide_r = jnp.concatenate([r, r], axis=1)
            head = rows[q][e : e + 1, :] * wide_r
            wide_c = jnp.concatenate([coef[q], coef[q]], axis=1)
            rows[q] = jnp.where(
                sub2 == e, head, jnp.where(sub2 > e, rows[q] - wide_c * head, rows[q])
            )
            for g in range(q + 1, n_part):
                wide_c = jnp.concatenate([coef[g], coef[g]], axis=1)
                rows[g] = rows[g] - wide_c * head
        done = jnp.concatenate(rows, axis=0)
        aug[pl.ds(j0, S), :] = done
        wide = lax.broadcasted_iota(jnp.int32, (S, T), 1)
        later = jnp.where(wide >= j0 + S, done[:, :T], 0.0)
        aug[...] -= dot6(left6(later, 0), right6(done), TN)
        return carry

    lax.fori_loop(0, T // S, strip, 0)


def split(x):
    top = x.astype(jnp.bfloat16)
    return top, (x - top.astype(jnp.float32)).astype(jnp.bfloat16)


def dot3(left, right, dims=NN):
    acc = None
    for a, b in ((left[1], right[0]), (left[0], right[1]), (left[0], right[0])):
        term = lax.dot_general(a, b, dims, preferred_element_type=jnp.float32)
        acc = term if acc is None else acc + term
    return acc


def kernel(
    shape, first, m_ref, o_ref,
    xs, mbuf, diag, work, aug, w, u01, ufix, cross, y0, y1, z0, bt, top, low,
    dsend, drecv, dloc, xsend, xrecv, csend, crecv, cloc, wsend, wrecv, mload, osend,
):
    n_row, n_col, n_dep = shape
    slots, block, _ = m_ref.shape
    held = slots - first
    half = block // 2
    n_dc = block // T
    n_pair = n_dep // 2
    r = lax.axis_index("row")
    c = lax.axis_index("col")
    d = lax.axis_index("depth")
    j = c * n_dep + d
    sib = d + 1 - 2 * lax.rem(d, 2)
    comm = lax.rem(d, 2) == lax.rem(r, 2)
    chain = jnp.logical_not(comm)
    kr = jnp.minimum(r, PANELS - 1)

    def dest(rr=None, cc=None, dd=None):
        return (r if rr is None else rr, c if cc is None else cc, d if dd is None else dd)

    def remote(src, dst, send, recv, to):
        return pltpu.make_async_remote_copy(
            src_ref=src, dst_ref=dst, send_sem=send, recv_sem=recv,
            device_id=to, device_id_type=MESH,
        )

    def chunks(n):
        if n == 1:
            return [(g * T, 0, block) for g in range(n_dc)]
        out = [(g * T, g * T, block - g * T) for g in range(n_dc)]
        if n == 0:
            out[:1] = [(0, 0, T), (0, T, block - T)]
        return out

    def diag_part(ref, n, g):
        at, col, wide = chunks(n)[g]
        return ref.at[pl.ds(at, T), pl.ds(col, wide)]

    def diag_copy(n, g, lane, to):
        part = diag_part(diag.at[n], n, g)
        return remote(part, part, dsend.at[n, g, lane], drecv.at[n, g], to)

    def diag_load(n, g):
        return pltpu.make_async_copy(
            diag_part(m_ref.at[0], n, g), diag_part(diag.at[n], n, g), dloc.at[n, g]
        )

    def diag_roles(n):
        row, k = DIAGS[n]
        root = (r == row) & (c == 0) & (d == k)
        own_entry = row % 2 == k % 2
        near = d < 2
        entry = comm & near & (c == 0) & (r == row)
        out = [(0, comm & near & (c < n_col - 1), dest(cc=lax.rem(c + 1, n_col)))]
        for q in range(1, n_pair):
            out.append((1 + q, comm & near, dest(dd=lax.rem(sib + 2 * q, n_dep))))
        for step in range(1, n_row):
            rr = lax.rem(r + step, n_row)
            out.append((n_pair + step, entry, dest(rr=rr, dd=lax.rem(rr, 2))))
        down = comm & near
        if not own_entry:
            down = (down & jnp.logical_not(entry)) | root
        out.insert(0, (1, down, dest(dd=sib)))
        rows = [x for x in out if x[0] > n_pair]
        rest = [x for x in out if x[0] <= n_pair]
        return root, rows + rest

    def diag_early(n):
        return DIAGS[n][0] % 2 == DIAGS[n][1] % 2

    def diag_rows(n):
        root, out = diag_roles(n)

        @pl.when(root)
        def _():
            for g in range(len(chunks(n))):
                diag_load(n, g).wait()
                for lane, cond, to in out:
                    if lane > n_pair:
                        diag_copy(n, g, lane, to).start()

    def diag_step(n, g):
        root, out = diag_roles(n)
        early = diag_early(n)

        @pl.when(root)
        def _():
            if not early:
                diag_load(n, g).wait()

        @pl.when(jnp.logical_not(root))
        def _():
            diag_copy(n, g, 0, dest(dd=sib)).wait_recv()

        for lane, cond, to in out:
            if early and lane > n_pair:
                continue

            @pl.when(cond)
            def _():
                diag_copy(n, g, lane, to).start()

    def diag_relay(n):
        for g in range(len(chunks(n))):
            diag_step(n, g)

    def diag_drain(n):
        _, out = diag_roles(n)
        for g in range(len(chunks(n))):
            for lane, cond, to in out:
                @pl.when(cond)
                def _():
                    diag_copy(n, g, lane, to).wait_send()

    def cross_copy(step):
        return remote(
            m_ref.at[0], cross.at[kr], csend.at[step - 1], crecv.at[kr],
            dest(rr=lax.rem(r + step, n_row)),
        )

    def cross_local():
        return pltpu.make_async_copy(m_ref.at[0], cross.at[kr], cloc.at[0])

    def cross_start():
        @pl.when(r < PANELS)
        def _():
            for step in range(1, n_row):
                cross_copy(step).start()

    def cross_wait(k):
        @pl.when(k == r)
        def _():
            cross_local().wait()

        @pl.when(k != r)
        def _():
            remote(
                m_ref.at[0], cross.at[k], csend.at[0], crecv.at[k],
                dest(rr=lax.rem(r + 1, n_row)),
            ).wait_recv()

    def piece(s, side, step):
        cs = c - side * s
        ds = lax.rem(d + 2 * step, n_dep)
        col = jnp.clip(cs, 0, n_col - 1) * n_dep + ds
        a = col // n_row
        ok = comm & (cs >= 0) & (cs < n_col) & (lax.rem(col, n_row) == r) & (a >= first)
        return ok, jnp.clip(a - first, 0, held - 1)

    def along(direction):
        out = []
        for t in range(1, n_col):
            cc = c + direction * t
            lane = (t - 1) if direction > 0 else (n_col - 2 + t)
            out.append((lane, (cc >= 0) & (cc < n_col), dest(cc=jnp.clip(cc, 0, n_col - 1))))
        return out

    def pairs():
        lane = 2 * (n_col - 1)
        return [(lane + q, c >= 0, dest(dd=lax.rem(d + 2 * q, n_dep))) for q in range(1, n_pair)]

    def down():
        return [(2 * (n_col - 1), c >= 0, dest(dd=sib))]

    def piece_out(s, step):
        if step:
            return down()
        return pairs() + down() + (along(-1) + along(1) if s == 0 else [])

    def x_part(k, a, h):
        size = block // H
        return xs.at[k, a, pl.ds(pl.multiple_of(h * size, size), size), :]

    def x_copy(k, a, h, lane, to):
        part = x_part(k, a, h)
        return remote(part, part, xsend.at[k, a, h, lane], xrecv.at[k, a, h], to)

    def x_send(k, out):
        ok, a = piece(0, 1, 0)

        @pl.when(ok)
        def _():
            def part(h, carry):
                for lane, cond, to in out:
                    @pl.when(cond)
                    def _():
                        x_copy(k, a, h, lane, to).start()
                return carry

            lax.fori_loop(0, H, part, 0)

    def x_event(s, side, step, k, h):
        ok, a = piece(s, side, step)

        @pl.when(ok)
        def _():
            x_copy(k, a, h, 0, dest(dd=sib)).wait_recv()
            for lane, cond, to in piece_out(s, step):
                x_copy(k, a, h, lane, to).start()

    def turn_of(e):
        return lax.rem(r + e // H, PANELS), lax.rem(e, H)

    def x_line(e):
        k, h = turn_of(e)
        for s, side in places[1:]:
            x_event(s, side, 0, k, h)

    def x_across(e):
        k, h = turn_of(e)
        for s, side in places:
            for step in range(1, n_pair):
                x_event(s, side, step, k, h)

    places = [(0, 1)] + [(s, side) for s in range(1, n_col) for side in (1, -1)]

    def x_own(k):
        ok, a = piece(0, 1, 0)

        @pl.when(ok)
        def _():
            def turn(e, carry):
                i = pl.multiple_of((e // n_dc) * T, T)
                l = pl.multiple_of(lax.rem(e, n_dc) * T, T)
                xs[k, a, pl.ds(l, T), pl.ds(i, T)] = cross[k, pl.ds(i, T), pl.ds(l, T)].T
                return carry

            lax.fori_loop(0, n_dc * n_dc, turn, 0)

    def x_drain():
        def one(e, carry):
            k = e // H
            h = lax.rem(e, H)
            for s, side in places:
                for step in range(n_pair):
                    ok, a = piece(s, side, step)
                    for lane, cond, to in piece_out(s, step):
                        @pl.when(ok & cond)
                        def _():
                            x_copy(k, a, h, lane, to).wait_send()
            return carry

        lax.fori_loop(0, H * PANELS, one, 0)

    def w_copy(panel, b):
        rows = pl.ds(pl.multiple_of(b * T, T), T)
        part = w.at[panel, rows, :]
        return remote(part, part, wsend.at[panel, b], wrecv.at[panel, b], dest(dd=sib))

    def u_copy():
        return remote(u01, u01, wsend.at[PANELS, 0], wrecv.at[PANELS, 0], dest(dd=sib))

    def fix_copy():
        return remote(ufix, ufix, wsend.at[PANELS, 1], wrecv.at[PANELS, 1], dest(dd=sib))

    def m_load(s):
        return pltpu.make_async_copy(m_ref.at[s + first], mbuf.at[s + first], mload.at[s])

    def all_loads(wait):
        def one(s, carry):
            if wait:
                m_load(s).wait()
            else:
                m_load(s).start()
            return carry

        lax.fori_loop(0, held, one, 0)

    for n, (row, k) in enumerate(DIAGS):
        @pl.when((d == k) & (c == 0) & (r == row))
        def _():
            for g in range(len(chunks(n))):
                diag_load(n, g).start()

    def eye(rows, columns, at):
        i = lax.broadcasted_iota(jnp.int32, (rows, columns), 0)
        l = lax.broadcasted_iota(jnp.int32, (rows, columns), 1)
        return jnp.where(i + at == l, jnp.float32(1.0), jnp.float32(0.0))

    def upper(x, at):
        i = lax.broadcasted_iota(jnp.int32, x.shape, 0)
        l = lax.broadcasted_iota(jnp.int32, x.shape, 1)
        return jnp.where(i + at <= l, x, 0.0)

    def lower(x, at):
        i = lax.broadcasted_iota(jnp.int32, x.shape, 0)
        l = lax.broadcasted_iota(jnp.int32, x.shape, 1)
        return jnp.where(i + at >= l, x, 0.0)

    def each_tile(f, size=T):
        def step(e, carry):
            f(pl.multiple_of(e * size, size))
            return carry

        lax.fori_loop(0, block // size, step, 0)

    def unit(k, x, at):
        i1 = lax.broadcasted_iota(jnp.int32, x.shape, 0)
        i2 = lax.broadcasted_iota(jnp.int32, x.shape, 1)
        minus = jnp.where((i1 + at == i2) & (j == k), jnp.float32(-1.0), 0.0)
        return jnp.where(j < PANELS, minus, x)

    def cut(ref, *index):
        return split(ref[index])

    def s1(at):
        rows = pl.ds(at, half)
        y0[rows, :] = unit(0, dot3(split(w[0, rows, :]), split(cross[0])), at)

    def s2(at):
        rows = pl.ds(at, half)
        y1[rows, :] = cross[1, rows, :] - dot3(split(u01[:, rows]), split(y0[...]), TN)

    def s3(at):
        rows = pl.ds(at, half)
        z0[rows, :] = dot3(split(w[0, :, rows]), split(y0[...]), TN)
        bt[rows, :] = dot3(split(w[0, :, rows]), split(u01[...]), TN)

    def early():
        each_tile(s1, half)
        each_tile(s2, half)
        each_tile(s3, half)

    def s4(at):
        rows = pl.ds(at, half)
        y0[rows, :] = unit(1, dot3(split(w[1, rows, :]), split(y1[...])), at)

    def s5(at):
        rows = pl.ds(at, half)
        value = dot3(split(w[1, :, rows]), split(y0[...]), TN)
        top[1, rows, :], low[1, rows, :] = split(value)

    def s6(at):
        rows = pl.ds(at, half)
        value = z0[rows, :] - dot3(split(bt[rows, :]), (top[1], low[1]))
        top[0, rows, :], low[0, rows, :] = split(value)

    def middle():
        each_tile(s4, half)
        each_tile(s5, half)
        each_tile(s6, half)

    def out_copy(s, h):
        rows = pl.ds(pl.multiple_of(h * (block // H), block // H), block // H)
        return pltpu.make_async_copy(mbuf.at[s, rows, :], o_ref.at[s, rows, :], osend.at[s, h])

    def update(h):
        rows = pl.ds(pl.multiple_of(h * (block // H), block // H), block // H)

        def one(a, carry):
            acc = jnp.where(j >= PANELS, mbuf[a + first, rows, :], 0.0)
            for k in range(PANELS):
                acc = acc - dot3(split(xs[k, a, rows, :]), (top[k], low[k]))
            if first:
                mbuf[a + first, rows, :] = acc
                out_copy(a + first, h).start()
            else:
                @pl.when((a > 0) | (r >= PANELS))
                def _():
                    mbuf[a, rows, :] = acc
                    out_copy(a, h).start()
            return carry

        lax.fori_loop(0, held, one, 0)

    def rest_of_update():
        def one(h, carry):
            update(h)
            return carry

        lax.fori_loop(2, H, one, 0)

    def corner():
        def turned(ref):
            def turn(e, carry):
                i = pl.multiple_of((e // n_dc) * T, T)
                l = pl.multiple_of(lax.rem(e, n_dc) * T, T)
                mbuf[0, pl.ds(l, T), pl.ds(i, T)] = ref[pl.ds(i, T), pl.ds(l, T)].T
                return carry

            lax.fori_loop(0, n_dc * n_dc, turn, 0)

        @pl.when(r < PANELS)
        def _():
            @pl.when(comm)
            def _():
                fix_copy().wait_recv()

            mbuf[0] = jnp.zeros((block, block), jnp.float32)

            @pl.when(j == r)
            def _():
                turned(ufix)

            @pl.when((j == 0) & (r == 1))
            def _():
                turned(u01)

            for h in range(H):
                out_copy(0, h).start()

    @pl.when(comm)
    def _():
        near = d < 2
        far = jnp.logical_not(near)
        head = near & (c == 0)
        for n in range(len(DIAGS)):
            if diag_early(n):
                diag_rows(n)

        @pl.when(r < PANELS)
        def _():
            cross_local().start()

        source, _ = piece(0, 1, 0)

        def own(kk):
            k = lax.rem(r + kk, PANELS)

            @pl.when(source)
            def _():
                cross_wait(k)
            x_own(k)
            x_send(k, down() + along(-1))

        def others(kk):
            x_send(lax.rem(r + kk, PANELS), pairs() + along(1))

        @pl.when(jnp.logical_not(head))
        def _():
            own(0)

        @pl.when(far)
        def _():
            others(0)

        @pl.when(near)
        def _():
            diag_relay(0)
            diag_relay(1)

            @pl.when(head)
            def _():
                own(0)
            x_send(lax.rem(r, PANELS), pairs())

        for kk in range(1, PANELS):
            own(kk)

        @pl.when(near)
        def _():
            diag_relay(2)
            x_send(lax.rem(r, PANELS), along(1))

        for kk in range(1, PANELS):
            others(kk)
        cross_start()

        all_loads(False)
        n_event = PANELS * H
        lead = n_event // 2

        def first_part(e, carry):
            x_line(e)
            return carry

        def second_part(e, carry):
            @pl.when(e == lead // 2)
            def _():
                @pl.when(jnp.logical_not(source))
                def _():
                    for k in range(PANELS):
                        cross_wait(jnp.int32(k))

                for b in range(n_dc):
                    w_copy(0, b).wait_recv()
                u_copy().wait_recv()
                early()

            @pl.when(e == lead - 1)
            def _():
                for b in range(n_dc):
                    w_copy(1, b).wait_recv()
                middle()
                all_loads(True)
                corner()
                update(0)

            x_line(lead + e)

            @pl.when(e > 0)
            def _():
                x_across(2 * e - 1)
            x_across(2 * e)
            return carry

        lax.fori_loop(0, lead, first_part, 0)
        lax.fori_loop(0, lead, second_part, 0)
        update(1)
        x_across(n_event - 1)
        rest_of_update()

    def factor_block(panel):
        def tile(b, carry):
            at = pl.multiple_of(b * T, T)
            rows = pl.ds(at, T)
            aug[:, :T] = work[rows, rows]
            aug[:, T:] = eye(T, T, 0)
            factor_tile(aug)
            if panel == 0:
                @pl.when(b == 0)
                def _():
                    for g in range(1, n_dc + 1):
                        diag_step(0, g)
                    each_tile(fill)
            line = dot6(left6(aug[:, T:], 1), right6(work[rows, :]))
            work[rows, :] = line
            w[panel, rows, :] = lower(line[:, block:], at)

            @pl.when(r == panel)
            def _():
                ufix[rows, :] = upper(line[:, :block], at)

            @pl.when(b < n_dc - 1)
            def _():
                lane = lax.broadcasted_iota(jnp.int32, (T, block), 1)
                aside = jnp.where(lane >= at + T, line[:, :block], 0.0)

                left = left6(aside, 0)

                def tail(e, carry2):
                    cols = pl.ds(pl.multiple_of(e * 2 * T, 2 * T), 2 * T)
                    work[:, cols] -= dot6(left, right6(work[rows, cols]), TN)
                    return carry2

                lax.fori_loop((b + 1) // 2, block // (2 * T) + b // 2 + 1, tail, 0)

            w_copy(panel, b).start()
            return carry

        lax.fori_loop(0, n_dc, tile, 0)

    def fill(at):
        rows = pl.ds(at, T)
        work[rows, :block] = diag[0, rows, :]
        work[rows, block:] = eye(T, block, at)

    def join(at):
        rows = pl.ds(at, T)
        u01[rows, :] = dot(w[0, rows, :], diag[1])

    def second(at):
        rows = pl.ds(at, T)
        work[rows, :block] = diag[2, rows, :] - dot(u01[:, rows], u01[...], TN)
        work[rows, block:] = eye(T, block, at)

    @pl.when(chain)
    def _():
        head = (d < 2) & (c == 0)

        @pl.when(r < PANELS)
        def _():
            cross_local().start()

        @pl.when(jnp.logical_not(head))
        def _():
            cross_start()

        diag_step(0, 0)
        work[pl.ds(0, T), pl.ds(0, T)] = diag[0, pl.ds(0, T), pl.ds(0, T)]
        all_loads(False)
        diag_start = DIAGS[1]

        @pl.when((r == diag_start[0]) & (c == 0) & (d == diag_start[1]))
        def _():
            diag_relay(1)

        factor_block(0)

        @pl.when(head)
        def _():
            cross_start()

        @pl.when(jnp.logical_not((r == diag_start[0]) & (c == 0) & (d == diag_start[1])))
        def _():
            diag_relay(1)

        each_tile(join)
        u_copy().start()
        diag_relay(2)
        each_tile(second)
        factor_block(1)
        for k in range(PANELS):
            cross_wait(jnp.int32(k))

        @pl.when(r < PANELS)
        def _():
            fix_copy().start()

        early()
        middle()
        all_loads(True)
        corner()

        def last(h, carry):
            def arrive(e, carry2):
                x_copy(e // held, lax.rem(e, held), h, 0, dest(dd=sib)).wait_recv()
                return carry2

            lax.fori_loop(0, PANELS * held, arrive, 0)
            update(h)
            return carry

        lax.fori_loop(0, H, last, 0)

    @pl.when(r < PANELS)
    def _():
        for step in range(1, n_row):
            cross_copy(step).wait_send()

    @pl.when(chain)
    def _():
        for panel in range(PANELS):
            for b in range(n_dc):
                w_copy(panel, b).wait_send()
        u_copy().wait_send()

        @pl.when(r < PANELS)
        def _():
            fix_copy().wait_send()

    for n in range(len(DIAGS)):
        diag_drain(n)
    x_drain()

    def finish(e, carry):
        out_copy(e // H, lax.rem(e, H)).wait()
        return carry

    lax.fori_loop(0, H * slots, finish, 0)


def body(shape, matrix):
    n_row, n_col, n_dep = shape
    m = matrix.reshape(matrix.shape[0], matrix.shape[2], matrix.shape[3])
    slots, block, _ = m.shape
    first = 1 if n_row <= PANELS else 0
    held = slots - first
    n_dc = block // T
    n_pair = n_dep // 2
    f32 = jnp.float32
    dma = pltpu.SemaphoreType.DMA
    hbm = pl.BlockSpec(memory_space=pltpu.HBM)
    square = pltpu.VMEM((block, block), f32)
    out = pl.pallas_call(
        functools.partial(kernel, shape, first),
        out_shape=jax.ShapeDtypeStruct(m.shape, f32),
        in_specs=[hbm],
        out_specs=pl.BlockSpec(memory_space=pl.ANY),
        scratch_shapes=[
            pltpu.VMEM((PANELS, held, block, block), f32),
            pltpu.VMEM((slots, block, block), f32),
            pltpu.VMEM((len(DIAGS), block, block), f32),
            pltpu.VMEM((block, 2 * block), f32),
            pltpu.VMEM((T, 2 * T), f32),
            pltpu.VMEM((PANELS, block, block), f32),
            square, square,
            pltpu.VMEM((PANELS, block, block), f32),
            square, square, square, square,
            pltpu.VMEM((PANELS, block, block), jnp.bfloat16),
            pltpu.VMEM((PANELS, block, block), jnp.bfloat16),
            dma((len(DIAGS), n_dc + 1, n_pair + n_row)),
            dma((len(DIAGS), n_dc + 1)),
            dma((len(DIAGS), n_dc + 1)),
            dma((PANELS, held, H, 2 * (n_col - 1) + n_pair)),
            dma((PANELS, held, H)),
            dma((n_row - 1,)),
            dma((PANELS,)),
            dma((1,)),
            dma((PANELS + 1, n_dc)),
            dma((PANELS + 1, n_dc)),
            dma((held,)),
            dma((slots, H)),
        ],
        compiler_params=pltpu.CompilerParams(has_side_effects=True, vmem_limit_bytes=44 << 20),
    )(m)
    return out.reshape(matrix.shape)


def solution(mesh):
    shape = (mesh.shape["row"], mesh.shape["col"], mesh.shape["depth"])
    placed = P(None, "row", None, ("col", "depth"))
    return jax.shard_map(
        functools.partial(body, shape),
        mesh=mesh,
        in_specs=(placed,),
        out_specs=placed,
        check_vma=False,
    )
```

```python
import functools

import jax
import jax.numpy as jnp
from jax import lax
from jax.experimental import pallas as pl
from jax.experimental.pallas import tpu as pltpu
from jax.sharding import PartitionSpec as P

PANELS = 2
MESH = pl.DeviceIdType.MESH
HI = lax.Precision.HIGHEST
T = 128
S = 16
H = 4
NT = (((1,), (1,)), ((), ()))
TN = (((0,), (0,)), ((), ()))
NN = (((1,), (0,)), ((), ()))
DIAGS = ((0, 0), (0, 1), (1, 1))


def dot(a, b, dims=NN):
    return lax.dot_general(a, b, dims, precision=HI, preferred_element_type=jnp.float32)


def stacked(x, order, axis):
    top = x.astype(jnp.bfloat16)
    rest = x - top.astype(jnp.float32)
    mid = rest.astype(jnp.bfloat16)
    low = (rest - mid.astype(jnp.float32)).astype(jnp.bfloat16)
    parts = (top, mid, low)
    return jnp.concatenate([parts[i] for i in order], axis=axis)


def left6(x, axis):
    return stacked(x, (1, 2, 0, 1, 0, 0), axis)


def right6(x, axis=0):
    return stacked(x, (1, 0, 2, 0, 1, 0), axis)


def dot6(left, right, dims=NN):
    return lax.dot_general(left, right, dims, preferred_element_type=jnp.float32)


def factor_tile(aug):
    n_part = S // 8

    def strip(i, carry):
        j0 = pl.multiple_of(i * S, S)
        rows = [aug[pl.ds(j0 + 8 * p, 8), :] for p in range(n_part)]
        lane = lax.broadcasted_iota(jnp.int32, (8, T), 1)
        sub = lax.broadcasted_iota(jnp.int32, (8, T), 0)
        sub2 = lax.broadcasted_iota(jnp.int32, (8, 2 * T), 0)
        cols = [
            [
                jnp.broadcast_to(
                    jnp.sum(jnp.where(lane == j0 + t, x[:, :T], 0.0), axis=1, keepdims=True), (8, T)
                )
                for t in range(S)
            ]
            for x in rows
        ]
        for t in range(S):
            q, e = t // 8, t % 8
            p = cols[q][t][e : e + 1, :]
            r = lax.rsqrt(p)
            r = r * (1.5 - 0.5 * p * r * r)
            coef = {g: cols[g][t] * r for g in range(q, n_part)}
            for u in range(t + 1, S):
                head = cols[q][u][e : e + 1, :] * r
                cols[q][u] = jnp.where(sub > e, cols[q][u] - coef[q] * head, cols[q][u])
                for g in range(q + 1, n_part):
                    cols[g][u] = cols[g][u] - coef[g] * head
            wide_r = jnp.concatenate([r, r], axis=1)
            head = rows[q][e : e + 1, :] * wide_r
            wide_c = jnp.concatenate([coef[q], coef[q]], axis=1)
            rows[q] = jnp.where(
                sub2 == e, head, jnp.where(sub2 > e, rows[q] - wide_c * head, rows[q])
            )
            for g in range(q + 1, n_part):
                wide_c = jnp.concatenate([coef[g], coef[g]], axis=1)
                rows[g] = rows[g] - wide_c * head
        done = jnp.concatenate(rows, axis=0)
        aug[pl.ds(j0, S), :] = done
        wide = lax.broadcasted_iota(jnp.int32, (S, T), 1)
        later = jnp.where(wide >= j0 + S, done[:, :T], 0.0)
        aug[...] -= dot6(left6(later, 0), right6(done), TN)
        return carry

    lax.fori_loop(0, T // S, strip, 0)


def split(x):
    top = x.astype(jnp.bfloat16)
    return top, (x - top.astype(jnp.float32)).astype(jnp.bfloat16)


def dot3(left, right, dims=NN):
    acc = None
    for a, b in ((left[1], right[0]), (left[0], right[1]), (left[0], right[0])):
        term = lax.dot_general(a, b, dims, preferred_element_type=jnp.float32)
        acc = term if acc is None else acc + term
    return acc


def kernel(
    shape, first, m_ref, o_ref,
    xs, mbuf, diag, work, aug, w, u01, ufix, cross, y0, y1, z0, bt, top, low,
    dsend, drecv, dloc, xsend, xrecv, csend, crecv, cloc, wsend, wrecv, mload, osend,
):
    n_row, n_col, n_dep = shape
    slots, block, _ = m_ref.shape
    held = slots - first
    half = block // 2
    n_dc = block // T
    n_pair = n_dep // 2
    r = lax.axis_index("row")
    c = lax.axis_index("col")
    d = lax.axis_index("depth")
    j = c * n_dep + d
    sib = d + 1 - 2 * lax.rem(d, 2)
    comm = lax.rem(d, 2) == lax.rem(r, 2)
    chain = jnp.logical_not(comm)
    kr = jnp.minimum(r, PANELS - 1)

    def dest(rr=None, cc=None, dd=None):
        return (r if rr is None else rr, c if cc is None else cc, d if dd is None else dd)

    def remote(src, dst, send, recv, to):
        return pltpu.make_async_remote_copy(
            src_ref=src, dst_ref=dst, send_sem=send, recv_sem=recv,
            device_id=to, device_id_type=MESH,
        )

    def chunks(n):
        if n == 1:
            return [(g * T, 0, block) for g in range(n_dc)]
        out = [(g * T, g * T, block - g * T) for g in range(n_dc)]
        if n == 0:
            out[:1] = [(0, 0, T), (0, T, block - T)]
        return out

    def diag_part(ref, n, g):
        at, col, wide = chunks(n)[g]
        return ref.at[pl.ds(at, T), pl.ds(col, wide)]

    def diag_copy(n, g, lane, to):
        part = diag_part(diag.at[n], n, g)
        return remote(part, part, dsend.at[n, g, lane], drecv.at[n, g], to)

    def diag_load(n, g):
        return pltpu.make_async_copy(
            diag_part(m_ref.at[0], n, g), diag_part(diag.at[n], n, g), dloc.at[n, g]
        )

    def diag_roles(n):
        row, k = DIAGS[n]
        root = (r == row) & (c == 0) & (d == k)
        own_entry = row % 2 == k % 2
        near = d < 2
        entry = comm & near & (c == 0) & (r == row)
        out = [(0, comm & near & (c < n_col - 1), dest(cc=lax.rem(c + 1, n_col)))]
        for q in range(1, n_pair):
            out.append((1 + q, comm & near, dest(dd=lax.rem(sib + 2 * q, n_dep))))
        for step in range(1, n_row):
            rr = lax.rem(r + step, n_row)
            out.append((n_pair + step, entry, dest(rr=rr, dd=lax.rem(rr, 2))))
        down = comm & near
        if not own_entry:
            down = (down & jnp.logical_not(entry)) | root
        out.insert(0, (1, down, dest(dd=sib)))
        rows = [x for x in out if x[0] > n_pair]
        rest = [x for x in out if x[0] <= n_pair]
        return root, rows + rest

    def diag_early(n):
        return DIAGS[n][0] % 2 == DIAGS[n][1] % 2

    def diag_rows(n):
        root, out = diag_roles(n)

        @pl.when(root)
        def _():
            for g in range(len(chunks(n))):
                diag_load(n, g).wait()
                for lane, cond, to in out:
                    if lane > n_pair:
                        diag_copy(n, g, lane, to).start()

    def diag_step(n, g):
        root, out = diag_roles(n)
        early = diag_early(n)

        @pl.when(root)
        def _():
            if not early:
                diag_load(n, g).wait()

        @pl.when(jnp.logical_not(root))
        def _():
            diag_copy(n, g, 0, dest(dd=sib)).wait_recv()

        for lane, cond, to in out:
            if early and lane > n_pair:
                continue

            @pl.when(cond)
            def _():
                diag_copy(n, g, lane, to).start()

    def diag_relay(n):
        for g in range(len(chunks(n))):
            diag_step(n, g)

    def diag_drain(n):
        _, out = diag_roles(n)
        for g in range(len(chunks(n))):
            for lane, cond, to in out:
                @pl.when(cond)
                def _():
                    diag_copy(n, g, lane, to).wait_send()

    def cross_copy(step):
        return remote(
            m_ref.at[0], cross.at[kr], csend.at[step - 1], crecv.at[kr],
            dest(rr=lax.rem(r + step, n_row)),
        )

    def cross_local():
        return pltpu.make_async_copy(m_ref.at[0], cross.at[kr], cloc.at[0])

    def cross_start():
        @pl.when(r < PANELS)
        def _():
            for step in range(1, n_row):
                cross_copy(step).start()

    def cross_wait(k):
        @pl.when(k == r)
        def _():
            cross_local().wait()

        @pl.when(k != r)
        def _():
            remote(
                m_ref.at[0], cross.at[k], csend.at[0], crecv.at[k],
                dest(rr=lax.rem(r + 1, n_row)),
            ).wait_recv()

    def piece(s, side, step):
        cs = c - side * s
        ds = lax.rem(d + 2 * step, n_dep)
        col = jnp.clip(cs, 0, n_col - 1) * n_dep + ds
        a = col // n_row
        ok = comm & (cs >= 0) & (cs < n_col) & (lax.rem(col, n_row) == r) & (a >= first)
        return ok, jnp.clip(a - first, 0, held - 1)

    def along(direction):
        out = []
        for t in range(1, n_col):
            cc = c + direction * t
            lane = (t - 1) if direction > 0 else (n_col - 2 + t)
            out.append((lane, (cc >= 0) & (cc < n_col), dest(cc=jnp.clip(cc, 0, n_col - 1))))
        return out

    def pairs():
        lane = 2 * (n_col - 1)
        return [(lane + q, c >= 0, dest(dd=lax.rem(d + 2 * q, n_dep))) for q in range(1, n_pair)]

    def down():
        return [(2 * (n_col - 1), c >= 0, dest(dd=sib))]

    def piece_out(s, step):
        if step:
            return down()
        return pairs() + down() + (along(-1) + along(1) if s == 0 else [])

    def x_part(k, a, h):
        size = block // H
        return xs.at[k, a, pl.ds(pl.multiple_of(h * size, size), size), :]

    def x_copy(k, a, h, lane, to):
        part = x_part(k, a, h)
        return remote(part, part, xsend.at[k, a, h, lane], xrecv.at[k, a, h], to)

    def x_send(k, out):
        ok, a = piece(0, 1, 0)

        @pl.when(ok)
        def _():
            def part(h, carry):
                for lane, cond, to in out:
                    @pl.when(cond)
                    def _():
                        x_copy(k, a, h, lane, to).start()
                return carry

            lax.fori_loop(0, H, part, 0)

    def x_event(s, side, step, k, h):
        ok, a = piece(s, side, step)

        @pl.when(ok)
        def _():
            x_copy(k, a, h, 0, dest(dd=sib)).wait_recv()
            for lane, cond, to in piece_out(s, step):
                x_copy(k, a, h, lane, to).start()

    def turn_of(e):
        return lax.rem(r + e // H, PANELS), lax.rem(e, H)

    def x_line(e):
        k, h = turn_of(e)
        for s, side in places[1:]:
            x_event(s, side, 0, k, h)

    def x_across(e):
        k, h = turn_of(e)
        for s, side in places:
            for step in range(1, n_pair):
                x_event(s, side, step, k, h)

    places = [(0, 1)] + [(s, side) for s in range(1, n_col) for side in (1, -1)]

    def x_own(k):
        ok, a = piece(0, 1, 0)

        @pl.when(ok)
        def _():
            def turn(e, carry):
                i = pl.multiple_of((e // n_dc) * T, T)
                l = pl.multiple_of(lax.rem(e, n_dc) * T, T)
                xs[k, a, pl.ds(l, T), pl.ds(i, T)] = cross[k, pl.ds(i, T), pl.ds(l, T)].T
                return carry

            lax.fori_loop(0, n_dc * n_dc, turn, 0)

    def x_drain():
        def one(e, carry):
            k = e // H
            h = lax.rem(e, H)
            for s, side in places:
                for step in range(n_pair):
                    ok, a = piece(s, side, step)
                    for lane, cond, to in piece_out(s, step):
                        @pl.when(ok & cond)
                        def _():
                            x_copy(k, a, h, lane, to).wait_send()
            return carry

        lax.fori_loop(0, H * PANELS, one, 0)

    def w_copy(panel, b):
        rows = pl.ds(pl.multiple_of(b * T, T), T)
        part = w.at[panel, rows, :]
        return remote(part, part, wsend.at[panel, b], wrecv.at[panel, b], dest(dd=sib))

    def u_copy():
        return remote(u01, u01, wsend.at[PANELS, 0], wrecv.at[PANELS, 0], dest(dd=sib))

    def fix_copy():
        return remote(ufix, ufix, wsend.at[PANELS, 1], wrecv.at[PANELS, 1], dest(dd=sib))

    def m_load(s):
        return pltpu.make_async_copy(m_ref.at[s + first], mbuf.at[s + first], mload.at[s])

    def all_loads(wait):
        def one(s, carry):
            if wait:
                m_load(s).wait()
            else:
                m_load(s).start()
            return carry

        lax.fori_loop(0, held, one, 0)

    for n, (row, k) in enumerate(DIAGS):
        @pl.when((d == k) & (c == 0) & (r == row))
        def _():
            for g in range(len(chunks(n))):
                diag_load(n, g).start()

    def eye(rows, columns, at):
        i = lax.broadcasted_iota(jnp.int32, (rows, columns), 0)
        l = lax.broadcasted_iota(jnp.int32, (rows, columns), 1)
        return jnp.where(i + at == l, jnp.float32(1.0), jnp.float32(0.0))

    def upper(x, at):
        i = lax.broadcasted_iota(jnp.int32, x.shape, 0)
        l = lax.broadcasted_iota(jnp.int32, x.shape, 1)
        return jnp.where(i + at <= l, x, 0.0)

    def lower(x, at):
        i = lax.broadcasted_iota(jnp.int32, x.shape, 0)
        l = lax.broadcasted_iota(jnp.int32, x.shape, 1)
        return jnp.where(i + at >= l, x, 0.0)

    def each_tile(f, size=T):
        def step(e, carry):
            f(pl.multiple_of(e * size, size))
            return carry

        lax.fori_loop(0, block // size, step, 0)

    def unit(k, x, at):
        i1 = lax.broadcasted_iota(jnp.int32, x.shape, 0)
        i2 = lax.broadcasted_iota(jnp.int32, x.shape, 1)
        minus = jnp.where((i1 + at == i2) & (j == k), jnp.float32(-1.0), 0.0)
        return jnp.where(j < PANELS, minus, x)

    def cut(ref, *index):
        return split(ref[index])

    def s1(at):
        rows = pl.ds(at, half)
        y0[rows, :] = unit(0, dot3(split(w[0, rows, :]), split(cross[0])), at)

    def s2(at):
        rows = pl.ds(at, half)
        y1[rows, :] = cross[1, rows, :] - dot3(split(u01[:, rows]), split(y0[...]), TN)

    def s3(at):
        rows = pl.ds(at, half)
        z0[rows, :] = dot3(split(w[0, :, rows]), split(y0[...]), TN)
        bt[rows, :] = dot3(split(w[0, :, rows]), split(u01[...]), TN)

    def early():
        each_tile(s1, half)
        each_tile(s2, half)
        each_tile(s3, half)

    def s4(at):
        rows = pl.ds(at, half)
        y0[rows, :] = unit(1, dot3(split(w[1, rows, :]), split(y1[...])), at)

    def s5(at):
        rows = pl.ds(at, half)
        value = dot3(split(w[1, :, rows]), split(y0[...]), TN)
        top[1, rows, :], low[1, rows, :] = split(value)

    def s6(at):
        rows = pl.ds(at, half)
        value = z0[rows, :] - dot3(split(bt[rows, :]), (top[1], low[1]))
        top[0, rows, :], low[0, rows, :] = split(value)

    def middle():
        each_tile(s4, half)
        each_tile(s5, half)
        each_tile(s6, half)

    def out_copy(s, h):
        rows = pl.ds(pl.multiple_of(h * (block // H), block // H), block // H)
        return pltpu.make_async_copy(mbuf.at[s, rows, :], o_ref.at[s, rows, :], osend.at[s, h])

    def update(h):
        rows = pl.ds(pl.multiple_of(h * (block // H), block // H), block // H)

        def one(a, carry):
            acc = jnp.where(j >= PANELS, mbuf[a + first, rows, :], 0.0)
            for k in range(PANELS):
                acc = acc - dot3(split(xs[k, a, rows, :]), (top[k], low[k]))
            if first:
                mbuf[a + first, rows, :] = acc
                out_copy(a + first, h).start()
            else:
                @pl.when((a > 0) | (r >= PANELS))
                def _():
                    mbuf[a, rows, :] = acc
                    out_copy(a, h).start()
            return carry

        lax.fori_loop(0, held, one, 0)

    def rest_of_update():
        def one(h, carry):
            update(h)
            return carry

        lax.fori_loop(3, H, one, 0)

    def corner():
        def turned(ref):
            def turn(e, carry):
                i = pl.multiple_of((e // n_dc) * T, T)
                l = pl.multiple_of(lax.rem(e, n_dc) * T, T)
                mbuf[0, pl.ds(l, T), pl.ds(i, T)] = ref[pl.ds(i, T), pl.ds(l, T)].T
                return carry

            lax.fori_loop(0, n_dc * n_dc, turn, 0)

        @pl.when(r < PANELS)
        def _():
            @pl.when(comm)
            def _():
                fix_copy().wait_recv()

            mbuf[0] = jnp.zeros((block, block), jnp.float32)

            @pl.when(j == r)
            def _():
                turned(ufix)

            @pl.when((j == 0) & (r == 1))
            def _():
                turned(u01)

            for h in range(H):
                out_copy(0, h).start()

    @pl.when(comm)
    def _():
        near = d < 2
        far = jnp.logical_not(near)
        head = near & (c == 0)
        for n in range(len(DIAGS)):
            if diag_early(n):
                diag_rows(n)

        @pl.when(r < PANELS)
        def _():
            cross_local().start()

        source, _ = piece(0, 1, 0)

        def own(kk):
            k = lax.rem(r + kk, PANELS)

            @pl.when(source)
            def _():
                cross_wait(k)
            x_own(k)
            x_send(k, down() + along(-1))

        def others(kk):
            x_send(lax.rem(r + kk, PANELS), pairs() + along(1))

        @pl.when(jnp.logical_not(head))
        def _():
            own(0)

        @pl.when(far)
        def _():
            others(0)

        @pl.when(near)
        def _():
            diag_relay(0)
            diag_relay(1)

            @pl.when(head)
            def _():
                own(0)
            x_send(lax.rem(r, PANELS), pairs())

        for kk in range(1, PANELS):
            own(kk)

        @pl.when(near)
        def _():
            diag_relay(2)
            x_send(lax.rem(r, PANELS), along(1))

        for kk in range(1, PANELS):
            others(kk)
        cross_start()

        all_loads(False)
        n_event = PANELS * H
        lead = n_event // 2

        def first_part(e, carry):
            x_line(e)
            return carry

        def second_part(e, carry):
            @pl.when(e == lead // 2)
            def _():
                @pl.when(jnp.logical_not(source))
                def _():
                    for k in range(PANELS):
                        cross_wait(jnp.int32(k))

                for b in range(n_dc):
                    w_copy(0, b).wait_recv()
                u_copy().wait_recv()
                early()

            @pl.when(e > 0)
            def _():
                x_across(2 * e - 1)

            @pl.when(e == lead - 1)
            def _():
                for b in range(n_dc):
                    w_copy(1, b).wait_recv()
                middle()
                all_loads(True)
                corner()
                update(0)
                update(1)

            x_line(lead + e)
            x_across(2 * e)
            return carry

        lax.fori_loop(0, lead, first_part, 0)
        lax.fori_loop(0, lead, second_part, 0)
        update(2)
        x_across(n_event - 1)
        rest_of_update()

    def factor_block(panel):
        def tile(b, carry):
            at = pl.multiple_of(b * T, T)
            rows = pl.ds(at, T)
            aug[:, :T] = work[rows, rows]
            aug[:, T:] = eye(T, T, 0)
            factor_tile(aug)
            if panel == 0:
                @pl.when(b == 0)
                def _():
                    for g in range(1, n_dc + 1):
                        diag_step(0, g)
                    each_tile(fill)
            line = dot6(left6(aug[:, T:], 1), right6(work[rows, :]))
            work[rows, :] = line
            w[panel, rows, :] = lower(line[:, block:], at)

            @pl.when(r == panel)
            def _():
                ufix[rows, :] = upper(line[:, :block], at)

            @pl.when(b < n_dc - 1)
            def _():
                lane = lax.broadcasted_iota(jnp.int32, (T, block), 1)
                aside = jnp.where(lane >= at + T, line[:, :block], 0.0)

                left = left6(aside, 0)

                def tail(e, carry2):
                    cols = pl.ds(pl.multiple_of(e * 2 * T, 2 * T), 2 * T)
                    work[:, cols] -= dot6(left, right6(work[rows, cols]), TN)
                    return carry2

                lax.fori_loop((b + 1) // 2, block // (2 * T) + b // 2 + 1, tail, 0)

            w_copy(panel, b).start()
            return carry

        lax.fori_loop(0, n_dc, tile, 0)

    def fill(at):
        rows = pl.ds(at, T)
        work[rows, :block] = diag[0, rows, :]
        work[rows, block:] = eye(T, block, at)

    def join(at):
        rows = pl.ds(at, T)
        u01[rows, :] = dot(w[0, rows, :], diag[1])

    def second(at):
        rows = pl.ds(at, T)
        work[rows, :block] = diag[2, rows, :] - dot(u01[:, rows], u01[...], TN)
        work[rows, block:] = eye(T, block, at)

    @pl.when(chain)
    def _():
        head = (d < 2) & (c == 0)

        @pl.when(r < PANELS)
        def _():
            cross_local().start()

        @pl.when(jnp.logical_not(head))
        def _():
            cross_start()

        diag_step(0, 0)
        work[pl.ds(0, T), pl.ds(0, T)] = diag[0, pl.ds(0, T), pl.ds(0, T)]
        all_loads(False)
        diag_start = DIAGS[1]

        @pl.when((r == diag_start[0]) & (c == 0) & (d == diag_start[1]))
        def _():
            diag_relay(1)

        factor_block(0)

        @pl.when(head)
        def _():
            cross_start()

        @pl.when(jnp.logical_not((r == diag_start[0]) & (c == 0) & (d == diag_start[1])))
        def _():
            diag_relay(1)

        each_tile(join)
        u_copy().start()
        diag_relay(2)
        each_tile(second)
        factor_block(1)
        for k in range(PANELS):
            cross_wait(jnp.int32(k))

        @pl.when(r < PANELS)
        def _():
            fix_copy().start()

        early()
        middle()
        all_loads(True)
        corner()

        def last(h, carry):
            def arrive(e, carry2):
                x_copy(e // held, lax.rem(e, held), h, 0, dest(dd=sib)).wait_recv()
                return carry2

            lax.fori_loop(0, PANELS * held, arrive, 0)
            update(h)
            return carry

        lax.fori_loop(0, H, last, 0)

    @pl.when(r < PANELS)
    def _():
        for step in range(1, n_row):
            cross_copy(step).wait_send()

    @pl.when(chain)
    def _():
        for panel in range(PANELS):
            for b in range(n_dc):
                w_copy(panel, b).wait_send()
        u_copy().wait_send()

        @pl.when(r < PANELS)
        def _():
            fix_copy().wait_send()

    for n in range(len(DIAGS)):
        diag_drain(n)
    x_drain()

    def finish(e, carry):
        out_copy(e // H, lax.rem(e, H)).wait()
        return carry

    lax.fori_loop(0, H * slots, finish, 0)


def body(shape, matrix):
    n_row, n_col, n_dep = shape
    m = matrix.reshape(matrix.shape[0], matrix.shape[2], matrix.shape[3])
    slots, block, _ = m.shape
    first = 1 if n_row <= PANELS else 0
    held = slots - first
    n_dc = block // T
    n_pair = n_dep // 2
    f32 = jnp.float32
    dma = pltpu.SemaphoreType.DMA
    hbm = pl.BlockSpec(memory_space=pltpu.HBM)
    square = pltpu.VMEM((block, block), f32)
    out = pl.pallas_call(
        functools.partial(kernel, shape, first),
        out_shape=jax.ShapeDtypeStruct(m.shape, f32),
        in_specs=[hbm],
        out_specs=pl.BlockSpec(memory_space=pl.ANY),
        scratch_shapes=[
            pltpu.VMEM((PANELS, held, block, block), f32),
            pltpu.VMEM((slots, block, block), f32),
            pltpu.VMEM((len(DIAGS), block, block), f32),
            pltpu.VMEM((block, 2 * block), f32),
            pltpu.VMEM((T, 2 * T), f32),
            pltpu.VMEM((PANELS, block, block), f32),
            square, square,
            pltpu.VMEM((PANELS, block, block), f32),
            square, square, square, square,
            pltpu.VMEM((PANELS, block, block), jnp.bfloat16),
            pltpu.VMEM((PANELS, block, block), jnp.bfloat16),
            dma((len(DIAGS), n_dc + 1, n_pair + n_row)),
            dma((len(DIAGS), n_dc + 1)),
            dma((len(DIAGS), n_dc + 1)),
            dma((PANELS, held, H, 2 * (n_col - 1) + n_pair)),
            dma((PANELS, held, H)),
            dma((n_row - 1,)),
            dma((PANELS,)),
            dma((1,)),
            dma((PANELS + 1, n_dc)),
            dma((PANELS + 1, n_dc)),
            dma((held,)),
            dma((slots, H)),
        ],
        compiler_params=pltpu.CompilerParams(has_side_effects=True, vmem_limit_bytes=44 << 20),
    )(m)
    return out.reshape(matrix.shape)


def solution(mesh):
    shape = (mesh.shape["row"], mesh.shape["col"], mesh.shape["depth"])
    placed = P(None, "row", None, ("col", "depth"))
    return jax.shard_map(
        functools.partial(body, shape),
        mesh=mesh,
        in_specs=(placed,),
        out_specs=placed,
        check_vma=False,
    )
```
